128 devices in a mesh: rep: 1, dp: 128 (over z, y, x, core).
Axes of the slice: x: 4, y: 4, z: 4, core: 2. Of those that a mesh axis runs over, the one named last changes fastest.
Arguments:
- hidden: bfloat16 [256, 2048], P(('rep', 'dp'))
- lengths: int32 [256], P(('rep', 'dp'))
- kv_cache: bfloat16 [2, 256, 512, 576], P(None, ('rep', 'dp'))
- norm_attn: float32 [2, 2048], replicated
- w_q: bfloat16 [2, 2048, 11520], replicated
- w_o: bfloat16 [2, 10240, 2048], replicated
- norm_ffn: float32 [2, 2048], replicated
- w_gate: bfloat16 [2, 2048, 10240], P(None, None, 'dp')
- w_up: bfloat16 [2, 2048, 10240], P(None, None, 'dp')
- w_down: bfloat16 [2, 10240, 2048], P(None, 'dp')
- norm_final: float32 [2048], replicated
- w_head: bfloat16 [2048, 154880], P(None, 'dp')
Outputs:
- output: float32 [256, 154880], P('rep', 'dp')
All inputs are finite; a program needn't handle non-finite values.
Results may differ from the reference program's by a relative error of at most 0.02.
Values are sent between devices in bfloat16 or wider.
A program may use at most 1 GiB of HBM per device.

```python
import jax
import jax.numpy as jnp
from jax import lax

BATCH_SIZE = 256
SEQ_LEN = 512
D_MODEL = 2048
NUM_HEADS = 20
FFN_DIM = 10240
VOCAB_SIZE = 154880
NUM_LAYERS = 2
LATENT_DIM = 512
ROPE_DIM = 64
KV_WIDTH = LATENT_DIM + ROPE_DIM
QK_SCALE = 192 ** -0.5
NORM_EPS = 1e-6


def setup_inputs(seed: int = 0, part: int = 0) -> dict:
    own_keys = jax.random.split(jax.random.fold_in(jax.random.key(seed), part), 3)
    shared_keys = jax.random.split(jax.random.key(seed + 1), 9)
    hidden = jax.random.normal(own_keys[0], (BATCH_SIZE, D_MODEL), jnp.float32)
    lengths = jax.random.randint(own_keys[1], (BATCH_SIZE,), 1, SEQ_LEN + 1, jnp.int32)
    lengths = lengths.at[0].set(SEQ_LEN)
    kv_cache = jax.random.normal(own_keys[2], (NUM_LAYERS, BATCH_SIZE, SEQ_LEN, KV_WIDTH), jnp.float32)
    attn_gain = SEQ_LEN ** 0.5 / 8.0
    norm_attn = jax.random.uniform(shared_keys[0], (NUM_LAYERS, D_MODEL), jnp.float32, 0.5, 1.5)
    w_q = jax.random.normal(shared_keys[1], (NUM_LAYERS, D_MODEL, NUM_HEADS * KV_WIDTH), jnp.float32) * D_MODEL ** -0.5
    w_o = jax.random.normal(shared_keys[2], (NUM_LAYERS, NUM_HEADS * LATENT_DIM, D_MODEL), jnp.float32) * ((NUM_HEADS * LATENT_DIM) ** -0.5 * attn_gain)
    norm_ffn = jax.random.uniform(shared_keys[3], (NUM_LAYERS, D_MODEL), jnp.float32, 0.5, 1.5)
    w_gate = jax.random.normal(shared_keys[4], (NUM_LAYERS, D_MODEL, FFN_DIM), jnp.float32) * D_MODEL ** -0.5
    w_up = jax.random.normal(shared_keys[5], (NUM_LAYERS, D_MODEL, FFN_DIM), jnp.float32) * D_MODEL ** -0.5
    w_down = jax.random.normal(shared_keys[6], (NUM_LAYERS, FFN_DIM, D_MODEL), jnp.float32) * (2.0 * FFN_DIM ** -0.5)
    norm_final = jax.random.uniform(shared_keys[7], (D_MODEL,), jnp.float32, 0.5, 1.5)
    w_head = jax.random.normal(shared_keys[8], (D_MODEL, VOCAB_SIZE), jnp.float32) * D_MODEL ** -0.5
    return dict(
        hidden=hidden.astype(jnp.bfloat16),
        lengths=lengths,
        kv_cache=kv_cache.astype(jnp.bfloat16),
        norm_attn=norm_attn,
        w_q=w_q.astype(jnp.bfloat16),
        w_o=w_o.astype(jnp.bfloat16),
        norm_ffn=norm_ffn,
        w_gate=w_gate.astype(jnp.bfloat16),
        w_up=w_up.astype(jnp.bfloat16),
        w_down=w_down.astype(jnp.bfloat16),
        norm_final=norm_final,
        w_head=w_head.astype(jnp.bfloat16),
    )


def rms_norm(x_rows, gain_vec):
    x_float = x_rows.astype(jnp.float32)
    inv_rms = lax.rsqrt(jnp.mean(x_float * x_float, axis=-1, keepdims=True) + NORM_EPS)
    return (x_float * inv_rms * gain_vec).astype(jnp.bfloat16)


def attend_row(row_args):
    q_heads, cache_row, length = row_args
    cache_float = cache_row.astype(jnp.float32)
    scores = jnp.dot(q_heads.astype(jnp.float32), cache_float.T, preferred_element_type=jnp.float32) * QK_SCALE
    key_valid = jnp.arange(cache_row.shape[0]) < length
    scores = jnp.where(key_valid[None, :], scores, -1e30)
    attn_probs = jax.nn.softmax(scores, axis=-1).astype(jnp.bfloat16)
    context = jnp.dot(attn_probs.astype(jnp.float32), cache_float[:, :LATENT_DIM], preferred_element_type=jnp.float32)
    return context.astype(jnp.bfloat16)


def reference(hidden, lengths, kv_cache, norm_attn, w_q, w_o, norm_ffn, w_gate, w_up, w_down, norm_final, w_head):
    num_rows = hidden.shape[0]

    def layer_step(x_rows, layer_args):
        layer_cache, attn_norm, wq_layer, wo_layer, ffn_norm, gate_layer, up_layer, down_layer = layer_args
        normed = rms_norm(x_rows, attn_norm)
        q_all = jnp.dot(normed, wq_layer, preferred_element_type=jnp.float32).astype(jnp.bfloat16)
        q_all = q_all.reshape(num_rows, NUM_HEADS, KV_WIDTH)
        context = lax.map(attend_row, (q_all, layer_cache, lengths)).reshape(num_rows, NUM_HEADS * LATENT_DIM)
        x_rows = (x_rows.astype(jnp.float32) + jnp.dot(context, wo_layer, preferred_element_type=jnp.float32)).astype(jnp.bfloat16)
        normed = rms_norm(x_rows, ffn_norm)
        gate_proj = jnp.dot(normed, gate_layer, preferred_element_type=jnp.float32)
        up_proj = jnp.dot(normed, up_layer, preferred_element_type=jnp.float32)
        act_rows = (jax.nn.silu(gate_proj) * up_proj).astype(jnp.bfloat16)
        ffn_out = jnp.dot(act_rows, down_layer, preferred_element_type=jnp.float32)
        x_rows = (x_rows.astype(jnp.float32) + ffn_out).astype(jnp.bfloat16)
        return x_rows, None

    layer_inputs = (kv_cache, norm_attn, w_q, w_o, norm_ffn, w_gate, w_up, w_down)
    x_final, layer_outs = lax.scan(layer_step, hidden, layer_inputs)
    normed = rms_norm(x_final, norm_final)
    return jnp.dot(normed, w_head, preferred_element_type=jnp.float32)
```

```python
import functools

import jax
import jax.numpy as jnp
from jax import lax
from jax.experimental import pallas as pl
from jax.experimental.pallas import tpu as pltpu
from jax.sharding import PartitionSpec as P

LATENT_DIM = 512
QK_SCALE = 192 ** -0.5
NORM_EPS = 1e-6
MESH = pl.DeviceIdType.MESH
VMEM_LIMIT = 60 * 1024 * 1024


def rms_norm(x_rows, gain_vec):
    x_float = x_rows.astype(jnp.float32)
    inv_rms = lax.rsqrt(jnp.mean(x_float * x_float, axis=-1, keepdims=True) + NORM_EPS)
    return (x_float * inv_rms * gain_vec).astype(jnp.bfloat16)


def mla_attention(normed, w_q, kv_cache, lengths):
    num_rows, seq_len, kv_width = kv_cache.shape
    q_heads = jnp.dot(normed, w_q, preferred_element_type=jnp.float32).astype(jnp.bfloat16)
    q_heads = q_heads.reshape(num_rows, -1, kv_width)
    scores = jnp.einsum('bhc,btc->bht', q_heads, kv_cache, preferred_element_type=jnp.float32) * QK_SCALE
    key_pos = lax.broadcasted_iota(jnp.int32, (1, 1, seq_len), 2)
    scores = jnp.where(key_pos < lengths[:, None, None], scores, -1e30)
    attn_probs = jax.nn.softmax(scores, axis=-1).astype(jnp.bfloat16)
    context = jnp.einsum('bht,btc->bhc', attn_probs, kv_cache[:, :, :LATENT_DIM], preferred_element_type=jnp.float32)
    return context.astype(jnp.bfloat16).reshape(num_rows, -1)


def ffn_block(normed, w_gate, w_up, w_down):
    gate_proj = jnp.dot(normed, w_gate, preferred_element_type=jnp.float32)
    up_proj = jnp.dot(normed, w_up, preferred_element_type=jnp.float32)
    act_rows = (jax.nn.silu(gate_proj) * up_proj).astype(jnp.bfloat16)
    return jnp.dot(act_rows, w_down, preferred_element_type=jnp.float32)


def add_residual(x_rows, delta):
    return (x_rows.astype(jnp.float32) + delta).astype(jnp.bfloat16)


def all_barrier(me, n):
    barrier = pltpu.get_barrier_semaphore()

    def signal(i, carry):
        pl.semaphore_signal(barrier, inc=1, device_id={'dp': lax.rem(me + i, n)}, device_id_type=MESH)
        return carry

    lax.fori_loop(1, n, signal, 0)
    pl.semaphore_wait(barrier, n - 1)


def gather_kernel(n, block_ref, out_ref, send_sem, recv_sem):
    me = lax.axis_index('dp')
    all_barrier(me, n)

    def send(i, carry):
        peer = lax.rem(me + i, n)
        pltpu.make_async_remote_copy(block_ref, out_ref.at[me], send_sem, recv_sem,
                                     device_id={'dp': peer}, device_id_type=MESH).start()
        return carry

    lax.fori_loop(1, n, send, 0)
    out_ref[me] = block_ref[...]
    others = out_ref.at[pl.ds(0, n - 1)]
    pltpu.make_async_copy(others, others, recv_sem).wait()
    pltpu.make_async_copy(others, others, send_sem).wait()


def scatter_kernel(n, part_ref, out_ref, land, send_sem, recv_sem):
    me = lax.axis_index('dp')
    all_barrier(me, n)

    def send(i, carry):
        peer = lax.rem(me + i, n)
        pltpu.make_async_remote_copy(part_ref.at[peer], land.at[me], send_sem, recv_sem,
                                     device_id={'dp': peer}, device_id_type=MESH).start()
        return carry

    lax.fori_loop(1, n, send, 0)
    land[me] = part_ref[me]
    others = land.at[pl.ds(0, n - 1)]
    pltpu.make_async_copy(others, others, recv_sem).wait()

    def add(i, total):
        return total + land[i]

    out_ref[...] = lax.fori_loop(1, n, add, land[0])
    pltpu.make_async_copy(others, others, send_sem).wait()


def comm_params(collective_id):
    return pltpu.CompilerParams(collective_id=collective_id, has_side_effects=True, vmem_limit_bytes=VMEM_LIMIT)


def gather_rows(block, n):
    rows, cols = block.shape
    return pl.pallas_call(
        functools.partial(gather_kernel, n),
        out_shape=jax.ShapeDtypeStruct((n, rows, cols), block.dtype),
        in_specs=[pl.BlockSpec(memory_space=pltpu.VMEM)],
        out_specs=pl.BlockSpec(memory_space=pltpu.VMEM),
        scratch_shapes=[pltpu.SemaphoreType.DMA, pltpu.SemaphoreType.DMA],
        compiler_params=comm_params(0),
    )(block).reshape(n * rows, cols)


def scatter_rows(part, n):
    rows, cols = part.shape[0] // n, part.shape[1]
    return pl.pallas_call(
        functools.partial(scatter_kernel, n),
        out_shape=jax.ShapeDtypeStruct((rows, cols), part.dtype),
        in_specs=[pl.BlockSpec(memory_space=pltpu.VMEM)],
        out_specs=pl.BlockSpec(memory_space=pltpu.VMEM),
        scratch_shapes=[pltpu.VMEM((n, rows, cols), part.dtype), pltpu.SemaphoreType.DMA, pltpu.SemaphoreType.DMA],
        compiler_params=comm_params(1),
    )(part.reshape(n, rows, cols))


def solution(mesh):
    row_axes = ('rep', 'dp')
    n = mesh.shape['dp']
    specs_in = (P(row_axes, None), P(row_axes), P(None, row_axes, None, None), P(), P(), P(), P(),
                P(None, None, 'dp'), P(None, None, 'dp'), P(None, 'dp', None), P(), P(None, 'dp'))

    def device_step(hidden, lengths, kv_cache, norm_attn, w_q, w_o, norm_ffn, w_gate, w_up, w_down, norm_final, w_head):
        x_rows = hidden
        for layer_idx in range(kv_cache.shape[0]):
            normed = rms_norm(x_rows, norm_attn[layer_idx])
            context = mla_attention(normed, w_q[layer_idx], kv_cache[layer_idx], lengths)
            x_rows = add_residual(x_rows, jnp.dot(context, w_o[layer_idx], preferred_element_type=jnp.float32))
            normed = rms_norm(x_rows, norm_ffn[layer_idx])
            gathered = gather_rows(normed, n)
            part_sum = ffn_block(gathered, w_gate[layer_idx], w_up[layer_idx], w_down[layer_idx])
            x_rows = add_residual(x_rows, scatter_rows(part_sum, n))
        normed = rms_norm(x_rows, norm_final)
        gathered = gather_rows(normed, n)
        return jnp.dot(gathered, w_head, preferred_element_type=jnp.float32)

    return jax.shard_map(device_step, mesh=mesh, in_specs=specs_in, out_specs=P('rep', 'dp'), check_vma=False)
```

```python
import jax
import jax.numpy as jnp
from jax import lax
from jax.experimental import pallas as pl
from jax.experimental.pallas import tpu as pltpu
from jax.sharding import PartitionSpec as P

MESH = pl.DeviceIdType.MESH
QK_SCALE = 192 ** -0.5
NORM_EPS = 1e-6

LAYERS = 2
ROWS = 2
TEAM = 8
TEAMS = 16
TEAM_ROWS = ROWS * TEAM
ALL_ROWS = TEAM_ROWS * TEAMS
D = 2048
D_OWN = D // TEAM
HEADS = 20
LATENT = 512
KV = 576
SEQ = 512
Q_COLS = HEADS * KV
Q_OWN = 1536
Q_LAST = Q_COLS - Q_OWN
PAIR = 2 * KV
PAIRS = HEADS // 2
SHIFT = 64
WIDE = KV + SHIFT
O_ROWS = 48
F_OWN = 80
F_TEAM = F_OWN * TEAM
F32 = jnp.float32
BF16 = jnp.bfloat16


def norm_rows(x, gain):
    inv_rms = lax.rsqrt(jnp.mean(x * x, axis=-1, keepdims=True) + NORM_EPS)
    return (x * inv_rms * gain).astype(BF16)


def dot_f32(a, b, contract=((1,), (0,))):
    return lax.dot_general(a, b, (contract, ((), ())), preferred_element_type=F32)


def wait_bytes(ref, sem):
    pltpu.make_async_copy(ref, ref, sem).wait()


def q_segments():
    pieces = []
    for pair in range(PAIRS):
        at, end = pair * PAIR, (pair + 1) * PAIR
        while at < end:
            sender = at // Q_OWN
            first = min(sender * Q_OWN, Q_LAST)
            stop = min(end, (sender + 1) * Q_OWN, Q_COLS)
            pieces.append((pair, at - pair * PAIR, sender, at - first, stop - at))
            at = stop
    return pieces


def decode_kernel(hidden, lengths, kv_cache, norm_attn, w_q, w_o, norm_ffn, w_gate, w_up, w_down, norm_final,
                  out, pack, spread, hid_send, hid_land, x_team, xb_team, wq_buf, kv_buf, wo_buf, wgu_buf, wd_buf,
                  q_send, q_land, q_pairs, o_send, o_land, o_heads, x_all, g_buf, a_all, part, land,
                  load_sem, entry_sem, send_sem, recv_sem, plane_sem, down_send, down_recv):
    me = lax.axis_index('dp')
    team, slot = me // TEAM, lax.rem(me, TEAM)
    plane, core = team // 4, lax.rem(me, 2)
    sibling = me + 1 - 2 * core
    own_cols = pl.ds(pl.multiple_of(slot * D_OWN, D_OWN), D_OWN)
    q_start = pl.multiple_of(jnp.minimum(slot * Q_OWN, Q_LAST), 128)

    def mate(i):
        return team * TEAM + lax.rem(slot + i, TEAM)

    def remote(src, dst, ssem, rsem, device):
        return pltpu.make_async_remote_copy(src, dst, ssem, rsem, device_id={'dp': device}, device_id_type=MESH)

    barrier = pltpu.get_barrier_semaphore()
    for i in range(1, TEAM):
        pl.semaphore_signal(barrier, inc=1, device_id={'dp': mate(i)}, device_id_type=MESH)

    def greet(i, carry):
        pl.semaphore_signal(barrier, inc=1, device_id={'dp': lax.rem(me + i * TEAM, TEAM * TEAMS)}, device_id_type=MESH)
        return carry

    lax.fori_loop(1, TEAMS, greet, 0)

    loads = []
    for layer in range(LAYERS):
        batch = [
            (w_q.at[layer, :, pl.ds(q_start, Q_OWN)], wq_buf.at[layer]),
            (kv_cache.at[layer], kv_buf.at[layer, :, pl.ds(SHIFT, KV)]),
            (w_o.at[layer, :, own_cols], wo_buf.at[layer]),
            (w_gate.at[layer], wgu_buf.at[layer, pl.ds(0, F_OWN)]),
            (w_up.at[layer], wgu_buf.at[layer, pl.ds(F_OWN, F_OWN)]),
            (w_down.at[layer, :, own_cols], wd_buf.at[layer, pl.ds(pl.multiple_of(slot * F_OWN, 16), F_OWN)]),
        ]
        loads.append([pltpu.make_async_copy(src, dst, load_sem.at[layer, i]) for i, (src, dst) in enumerate(batch)])
    for batch in loads:
        for copy in batch:
            copy.start()

    for layer in range(LAYERS):
        for r in range(ROWS):
            kv_buf[layer, r, 0:SHIFT, :] = jnp.zeros((SHIFT, SEQ), BF16)
            kv_buf[layer, r, SHIFT + KV:, :] = jnp.zeros((SHIFT, SEQ), BF16)
    q_pairs[...] = jnp.zeros_like(q_pairs)
    make_selectors(pack, spread)
    hid_send[...] = hidden[...].astype(F32)
    hid_land[slot] = hid_send[...]

    pl.semaphore_wait(barrier, TEAM - 1 + TEAMS - 1)
    for i in range(1, TEAM):
        pl.semaphore_signal(entry_sem, inc=1, device_id={'dp': mate(i)}, device_id_type=MESH)

    def gather_team(src, dst, sem):
        for i in range(1, TEAM):
            remote(src, dst, send_sem.at[sem], recv_sem.at[sem], mate(i)).start()

    def gather_all(block, step):
        dst = x_all.at[step]
        mine = dst.at[team, :, own_cols]
        mine[...] = block
        sem = 16 + 2 * step
        for dz in range(4):
            to_plane = lax.rem(plane + dz, 4)

            def send(i, carry):
                spot = lax.rem(lax.rem(me, 32) // 2 + i, 16)
                remote(mine, mine, send_sem.at[sem], plane_sem.at[step, (4 - dz) % 4],
                       to_plane * 32 + spot * 2 + core).start()
                return carry

            lax.fori_loop(1 if dz == 0 else 0, 16, send, 0)
        for dz in range(4):
            from_plane = lax.rem(plane + dz, 4)
            if dz == 0:
                wait_bytes(dst.at[0:3, :, 0:5 * D_OWN], plane_sem.at[step, dz])
            else:
                wait_bytes(dst.at[0:4, :, 0:4 * D_OWN], plane_sem.at[step, dz])
            for x in range(4):
                cols = pl.ds(pl.multiple_of((2 * x + core) * D_OWN, D_OWN), D_OWN)
                piece = dst.at[pl.ds(from_plane * 4, 4), :, cols]
                remote(piece, piece, send_sem.at[sem + 1], recv_sem.at[sem], sibling).start()
        wait_bytes(dst.at[0:8], recv_sem.at[sem])
        wait_bytes(dst.at[0:8], send_sem.at[sem + 1])
        wait_bytes(dst.at[0:7], send_sem.at[sem])
        wait_bytes(dst.at[0, :, 0:7 * D_OWN], send_sem.at[sem])

    def norm_all(step, gain):
        def chunk(i, carry):
            g_buf[pl.ds(pl.multiple_of(i * TEAM_ROWS, TEAM_ROWS), TEAM_ROWS), :] = norm_rows(
                x_all[step, i].astype(F32), gain)
            return carry

        lax.fori_loop(0, TEAMS, chunk, 0)

    gather_team(hid_send, hid_land.at[slot], 0)
    wait_bytes(hid_land.at[0:TEAM - 1], recv_sem.at[0])
    for i in range(TEAM):
        x_team[ROWS * i:ROWS * (i + 1), :] = hid_land[i]

    for layer in range(LAYERS):
        base = 8 * layer
        h = norm_rows(x_team[...], norm_attn[layer:layer + 1, :])
        x_block = x_team[:, own_cols]
        loads[layer][0].wait()
        for c in range(Q_OWN // 256):
            cols = slice(c * 256, (c + 1) * 256)
            q = dot_f32(h, wq_buf[layer, :, cols])
            for i in range(TEAM):
                q_send[layer, i, :, cols] = q[ROWS * i:ROWS * (i + 1), :]
        for i in range(1, TEAM):
            to = lax.rem(slot + i, TEAM)
            remote(q_send.at[layer, to], q_land.at[layer, slot], send_sem.at[base + 1], recv_sem.at[base + 1],
                   mate(i)).start()
        for i in range(1, TEAM):
            to = lax.rem(slot + i, TEAM)
            remote(w_down.at[layer, :, pl.ds(pl.multiple_of(to * D_OWN, D_OWN), D_OWN)],
                   wd_buf.at[layer, pl.ds(pl.multiple_of(slot * F_OWN, 16), F_OWN)],
                   down_send.at[layer], down_recv.at[layer], mate(i)).start()
        q_land[layer, slot] = q_send[layer, slot]
        wait_bytes(q_land.at[layer, 0:TEAM - 1], recv_sem.at[base + 1])
        for pair, at, sender, col, width in q_segments():
            for r in range(ROWS):
                q_pairs[r, pair:pair + 1, at:at + width] = q_land[layer, sender, r:r + 1, col:col + width]

        loads[layer][1].wait()
        lane = lax.broadcasted_iota(jnp.int32, (16, WIDE), 1)
        key_pos = lax.broadcasted_iota(jnp.int32, (32, SEQ), 1)
        contexts = []
        for r in range(ROWS):
            q_even = jnp.where(lane < KV, q_pairs[r, :, 0:WIDE], 0.0).astype(BF16)
            q_odd = jnp.where(lane >= SHIFT, q_pairs[r, :, PAIR - WIDE:PAIR], 0.0).astype(BF16)
            scores = jnp.concatenate([dot_f32(q_even, kv_buf[layer, r, SHIFT:SHIFT + WIDE, :]),
                                      dot_f32(q_odd, kv_buf[layer, r, 0:WIDE, :])], axis=0) * QK_SCALE
            scores = jnp.where(key_pos < lengths[r], scores, -1e30)
            weights = jnp.exp(scores - jnp.max(scores, axis=-1, keepdims=True))
            probs = (weights / jnp.sum(weights, axis=-1, keepdims=True)).astype(BF16)
            contexts.append(dot_f32(probs, kv_buf[layer, r, SHIFT:SHIFT + LATENT, :], ((1,), (1,))).astype(BF16))
        o_send[layer] = dot_f32(pack[...], jnp.concatenate(contexts, axis=0)).astype(BF16)
        gather_team(o_send.at[layer], o_land.at[layer, slot], base + 2)
        o_land[layer, slot] = o_send[layer]
        wait_bytes(o_land.at[layer, 0:TEAM - 1], recv_sem.at[base + 2])

        o_heads[...] = dot_f32(spread[...], o_land[layer].reshape(TEAM * O_ROWS, LATENT)).astype(BF16)
        loads[layer][2].wait()

        def head(i, total):
            return total + dot_f32(o_heads[pl.ds(pl.multiple_of(i * TEAM_ROWS, TEAM_ROWS), TEAM_ROWS), :],
                                   wo_buf[layer, pl.ds(pl.multiple_of(i * LATENT, LATENT), LATENT), :])

        delta = lax.fori_loop(0, HEADS, head, jnp.zeros((TEAM_ROWS, D_OWN), F32))
        x_block = (x_block + delta).astype(BF16)
        if layer == 0:
            pl.semaphore_wait(entry_sem, TEAM - 1)
        gather_all(x_block, layer)

        norm_all(layer, norm_ffn[layer:layer + 1, :])
        loads[layer][3].wait()
        loads[layer][4].wait()
        gate_up = dot_f32(wgu_buf[layer], g_buf[...], ((1,), (1,)))
        act = (jax.nn.silu(gate_up[0:F_OWN]) * gate_up[F_OWN:]).astype(BF16)
        own_hidden = a_all.at[layer, pl.ds(pl.multiple_of(slot * F_OWN, 16), F_OWN)]
        own_hidden[...] = act
        gather_team(own_hidden, own_hidden, base + 3)
        wait_bytes(a_all.at[layer, 0:F_TEAM - F_OWN], recv_sem.at[base + 3])
        loads[layer][5].wait()
        wait_bytes(wd_buf.at[layer, 0:F_TEAM - F_OWN], down_recv.at[layer])
        part[layer] = dot_f32(a_all[layer], wd_buf[layer], ((0,), (0,))).reshape(TEAMS, TEAM_ROWS, D_OWN)

        def scatter(i, carry):
            to = lax.rem(team + i, TEAMS)
            remote(part.at[layer, to], land.at[layer, team], send_sem.at[base + 4], recv_sem.at[base + 4],
                   to * TEAM + slot).start()
            return carry

        lax.fori_loop(1, TEAMS, scatter, 0)
        land[layer, team] = part[layer, team]
        wait_bytes(land.at[layer, 0:TEAMS - 1], recv_sem.at[base + 4])
        total = land[layer, 0]
        for i in range(1, TEAMS):
            total = total + land[layer, i]
        x_block = (x_block.astype(F32) + total).astype(BF16)

        wait_bytes(q_land.at[layer, 0:TEAM - 1], send_sem.at[base + 1])
        wait_bytes(o_land.at[layer, 0:TEAM - 1], send_sem.at[base + 2])
        wait_bytes(a_all.at[layer, 0:F_TEAM - F_OWN], send_sem.at[base + 3])
        wait_bytes(land.at[layer, 0:TEAMS - 1], send_sem.at[base + 4])
        wait_bytes(wd_buf.at[layer, 0:F_TEAM - F_OWN], down_send.at[layer])
        if layer == 0:
            wait_bytes(hid_land.at[0:TEAM - 1], send_sem.at[0])
            own_block = xb_team.at[:, own_cols]
            own_block[...] = x_block
            gather_team(own_block, own_block, 5)
            wait_bytes(xb_team.at[:, 0:D - D_OWN], recv_sem.at[5])
            x_team[...] = xb_team[...].astype(F32)
            wait_bytes(xb_team.at[:, 0:D - D_OWN], send_sem.at[5])
        else:
            gather_all(x_block, LAYERS)

    norm_all(LAYERS, norm_final[...])
    out[...] = g_buf[...]


def make_selectors(pack, spread):
    row = lax.broadcasted_iota(jnp.int32, pack.shape, 0)
    col = lax.broadcasted_iota(jnp.int32, pack.shape, 1)
    seq = jnp.where(row >= HEADS, 1, 0)
    head = row - HEADS * seq
    hit = (col == seq * 32 + (head & 1) * 16 + (head >> 1)) & (row < ROWS * HEADS)
    pack[...] = jnp.where(hit, 1.0, 0.0).astype(BF16)
    shape = (TEAM_ROWS, TEAM * O_ROWS)
    row = lax.broadcasted_iota(jnp.int32, shape, 0)
    col = lax.broadcasted_iota(jnp.int32, shape, 1)
    head = col - (row >> 1) * O_ROWS - (row & 1) * HEADS
    for i in range(HEADS):
        spread[i * TEAM_ROWS:(i + 1) * TEAM_ROWS, :] = jnp.where(head == i, 1.0, 0.0).astype(BF16)


def decode(hidden, lengths, kv_cache, norm_attn, w_q, w_o, norm_ffn, w_gate, w_up, w_down, norm_final):
    vmem = pl.BlockSpec(memory_space=pltpu.VMEM)
    smem = pl.BlockSpec(memory_space=pltpu.SMEM)
    hbm = pl.BlockSpec(memory_space=pl.ANY)
    dma = pltpu.SemaphoreType.DMA
    return pl.pallas_call(
        decode_kernel,
        out_shape=jax.ShapeDtypeStruct((ALL_ROWS, D), BF16),
        in_specs=[vmem, smem, hbm, vmem, hbm, hbm, vmem, hbm, hbm, hbm, vmem],
        out_specs=vmem,
        scratch_shapes=[
            pltpu.VMEM((O_ROWS, 64), BF16),
            pltpu.VMEM((HEADS * TEAM_ROWS, TEAM * O_ROWS), BF16),
            pltpu.VMEM((ROWS, D), F32),
            pltpu.VMEM((TEAM, ROWS, D), F32),
            pltpu.VMEM((TEAM_ROWS, D), F32),
            pltpu.VMEM((TEAM_ROWS, D), BF16),
            pltpu.VMEM((LAYERS, D, Q_OWN), BF16),
            pltpu.VMEM((LAYERS, ROWS, KV + 2 * SHIFT, SEQ), BF16),
            pltpu.VMEM((LAYERS, HEADS * LATENT, D_OWN), BF16),
            pltpu.VMEM((LAYERS, 2 * F_OWN, D), BF16),
            pltpu.VMEM((LAYERS, F_TEAM, D_OWN), BF16),
            pltpu.VMEM((LAYERS, TEAM, ROWS, Q_OWN), F32),
            pltpu.VMEM((LAYERS, TEAM, ROWS, Q_OWN), F32),
            pltpu.VMEM((ROWS, 16, PAIR), F32),
            pltpu.VMEM((LAYERS, O_ROWS, LATENT), BF16),
            pltpu.VMEM((LAYERS, TEAM, O_ROWS, LATENT), BF16),
            pltpu.VMEM((HEADS * TEAM_ROWS, LATENT), BF16),
            pltpu.VMEM((LAYERS + 1, TEAMS, TEAM_ROWS, D), BF16),
            pltpu.VMEM((ALL_ROWS, D), BF16),
            pltpu.VMEM((LAYERS, F_TEAM, ALL_ROWS), BF16),
            pltpu.VMEM((LAYERS, TEAMS, TEAM_ROWS, D_OWN), F32),
            pltpu.VMEM((LAYERS, TEAMS, TEAM_ROWS, D_OWN), F32),
            dma((LAYERS, 6)),
            pltpu.SemaphoreType.REGULAR,
            dma((22,)),
            dma((22,)),
            dma((LAYERS + 1, 4)),
            dma((LAYERS,)),
            dma((LAYERS,)),
        ],
        compiler_params=pltpu.CompilerParams(collective_id=0, has_side_effects=True, vmem_limit_bytes=60 * 1024 * 1024),
        name='decode',
    )(hidden, lengths, kv_cache, norm_attn, w_q, w_o, norm_ffn, w_gate, w_up, w_down, norm_final)


def solution(mesh):
    row_axes = ('rep', 'dp')
    specs_in = (P(row_axes, None), P(row_axes), P(None, row_axes, None, None), P(), P(), P(), P(),
                P(None, None, 'dp'), P(None, None, 'dp'), P(None, 'dp', None), P(), P(None, 'dp'))

    def device_step(hidden, lengths, kv_cache, norm_attn, w_q, w_o, norm_ffn, w_gate, w_up, w_down, norm_final, w_head):
        normed = decode(hidden, lengths, jnp.swapaxes(kv_cache, 2, 3), norm_attn, w_q, w_o, norm_ffn,
                        jnp.swapaxes(w_gate, 1, 2), jnp.swapaxes(w_up, 1, 2), w_down, norm_final.reshape(1, -1))
        return jnp.dot(normed, w_head, preferred_element_type=jnp.float32)

    return jax.shard_map(device_step, mesh=mesh, in_specs=specs_in, out_specs=P('rep', 'dp'), check_vma=False)
```

```python
import jax
import jax.numpy as jnp
from jax import lax
from jax.experimental import pallas as pl
from jax.experimental.pallas import tpu as pltpu
from jax.sharding import PartitionSpec as P

MESH = pl.DeviceIdType.MESH
QK_SCALE = 192 ** -0.5
NORM_EPS = 1e-6

LAYERS = 2
ROWS = 2
TEAM = 8
TEAMS = 16
TEAM_ROWS = ROWS * TEAM
ALL_ROWS = TEAM_ROWS * TEAMS
D = 2048
D_OWN = D // TEAM
HEADS = 20
LATENT = 512
KV = 576
SEQ = 512
Q_COLS = HEADS * KV
Q_OWN = 1536
Q_LAST = Q_COLS - Q_OWN
PAIR = 2 * KV
PAIRS = HEADS // 2
SHIFT = 64
WIDE = KV + SHIFT
O_ROWS = 24
F_OWN = 80
F_TEAM = F_OWN * TEAM
VOCAB_OWN = 1210
HEAD_CHUNK = 304
F32 = jnp.float32
BF16 = jnp.bfloat16


def norm_rows(x, gain):
    inv_rms = lax.rsqrt(jnp.mean(x * x, axis=-1, keepdims=True) + NORM_EPS)
    return (x * inv_rms * gain).astype(BF16)


def dot_f32(a, b, contract=((1,), (0,))):
    return lax.dot_general(a, b, (contract, ((), ())), preferred_element_type=F32)


def wait_bytes(ref, sem):
    pltpu.make_async_copy(ref, ref, sem).wait()


def q_segments():
    pieces = []
    for pair in range(PAIRS):
        at, end = pair * PAIR, (pair + 1) * PAIR
        while at < end:
            sender = at // Q_OWN
            first = min(sender * Q_OWN, Q_LAST)
            stop = min(end, (sender + 1) * Q_OWN, Q_COLS)
            pieces.append((pair, at - pair * PAIR, sender, at - first, stop - at))
            at = stop
    return pieces


def decode_kernel(hidden, lengths, kv_cache, norm_attn, w_q, w_o, norm_ffn, w_gate, w_up, w_down, norm_final, w_head,
                  out, head_buf, logits, pack, spread, hid_send, hid_land, x_team, xb_team, wq_buf, kv_buf, wo_buf, wgu_buf, wd_buf,
                  q_send, q_land, q_pairs, o_send, o_land, o_heads, x_all, g_buf, a_all, part, land,
                  load_sem, entry_sem, send_sem, recv_sem, plane_sem, down_send, down_recv, head_sem, out_sem):
    me = lax.axis_index('dp')
    team, slot = me // TEAM, lax.rem(me, TEAM)
    plane, core = team // 4, lax.rem(me, 2)
    sibling = me + 1 - 2 * core
    own_cols = pl.ds(pl.multiple_of(slot * D_OWN, D_OWN), D_OWN)
    q_start = pl.multiple_of(jnp.minimum(slot * Q_OWN, Q_LAST), 128)

    pending = []

    def take(layer, i):
        loads[layer][i].wait()

    def mate(i):
        return team * TEAM + lax.rem(slot + i, TEAM)

    def remote(src, dst, ssem, rsem, device):
        return pltpu.make_async_remote_copy(src, dst, ssem, rsem, device_id={'dp': device}, device_id_type=MESH)

    barrier = pltpu.get_barrier_semaphore()
    for i in range(1, TEAM):
        pl.semaphore_signal(barrier, inc=1, device_id={'dp': mate(i)}, device_id_type=MESH)

    def greet(i, carry):
        pl.semaphore_signal(barrier, inc=1, device_id={'dp': lax.rem(me + i * TEAM, TEAM * TEAMS)}, device_id_type=MESH)
        return carry

    lax.fori_loop(1, TEAMS, greet, 0)

    loads = []
    for layer in range(LAYERS):
        batch = [
            (w_q.at[layer, :, pl.ds(q_start, Q_OWN)], wq_buf.at[layer]),
            (kv_cache.at[layer], kv_buf.at[layer, :, pl.ds(SHIFT, KV)]),
            (w_o.at[layer, :, own_cols], wo_buf.at[layer]),
            (w_gate.at[layer], wgu_buf.at[layer, pl.ds(0, F_OWN)]),
            (w_up.at[layer], wgu_buf.at[layer, pl.ds(F_OWN, F_OWN)]),
            (w_down.at[layer, :, own_cols], wd_buf.at[layer, pl.ds(pl.multiple_of(slot * F_OWN, 16), F_OWN)]),
        ]
        loads.append([pltpu.make_async_copy(src, dst, load_sem.at[layer, i]) for i, (src, dst) in enumerate(batch)])
    for batch in loads:
        for copy in batch:
            copy.start()
    head_load = pltpu.make_async_copy(w_head, head_buf, head_sem)
    head_load.start()

    for layer in range(LAYERS):
        for r in range(ROWS):
            kv_buf[layer, r, 0:SHIFT, :] = jnp.zeros((SHIFT, SEQ), BF16)
            kv_buf[layer, r, SHIFT + KV:, :] = jnp.zeros((SHIFT, SEQ), BF16)
    q_pairs[...] = jnp.zeros_like(q_pairs)
    make_selectors(pack, spread)
    hid_send[...] = hidden[...].astype(F32)
    hid_land[slot] = hid_send[...]

    pl.semaphore_wait(barrier, TEAM - 1 + TEAMS - 1)
    for i in range(1, TEAM):
        pl.semaphore_signal(entry_sem, inc=1, device_id={'dp': mate(i)}, device_id_type=MESH)

    def gather_team(src, dst, sem):
        for i in range(1, TEAM):
            remote(src, dst, send_sem.at[sem], recv_sem.at[sem], mate(i)).start()
            pending.append((src, send_sem.at[sem]))

    def share_down(layer):
        for i in range(1, TEAM):
            to = lax.rem(slot + i, TEAM)
            remote(w_down.at[layer, :, pl.ds(pl.multiple_of(to * D_OWN, D_OWN), D_OWN)],
                   wd_buf.at[layer, pl.ds(pl.multiple_of(slot * F_OWN, 16), F_OWN)],
                   down_send.at[layer], down_recv.at[layer], mate(i)).start()
        pending.append((wd_buf.at[layer, 0:F_TEAM - F_OWN], down_send.at[layer]))

    def gather_all(block, step, gain):
        dst = x_all.at[step]
        mine = dst.at[team, :, own_cols]
        mine[...] = block
        direct, passed = send_sem.at[16 + 2 * step], send_sem.at[17 + 2 * step]
        planes = (plane, plane + 1 - 2 * lax.rem(plane, 2), 3 - plane, lax.rem(plane + 2, 4))
        for k in (3, 2, 1, 0):

            def send(i, carry, k=k):
                spot = lax.rem(lax.rem(me, 32) // 2 + 24 - i, 16)
                remote(mine, mine, direct, plane_sem.at[step, k], planes[k] * 32 + spot * 2 + core).start()
                return carry

            def send_near(i, carry, k=k):
                spot = lax.rem(lax.rem(me, 32) // 2 + i, 16)
                remote(mine, mine, direct, plane_sem.at[step, k], planes[k] * 32 + spot * 2 + core).start()
                return carry

            if k:
                lax.fori_loop(0, 16, send, 0)
            else:
                lax.fori_loop(1, 16, send_near, 0)
        pending.append((dst.at[0:7], direct))
        pending.append((dst.at[0, :, 0:7 * D_OWN], direct))
        pending.append((dst.at[0:8], passed))

        def finish(k):
            wait_bytes(dst.at[0:4, :, 0:4 * D_OWN], plane_sem.at[step, 4 + k])

            def chunk(i, carry):
                row = planes[k] * 4 + i
                g_buf[pl.ds(pl.multiple_of(row * TEAM_ROWS, TEAM_ROWS), TEAM_ROWS), :] = norm_rows(
                    dst[row].astype(F32), gain)
                return carry

            lax.fori_loop(0, 4, chunk, 0)

        for k in range(4):
            if k == 0:
                wait_bytes(dst.at[0:3, :, 0:5 * D_OWN], plane_sem.at[step, k])
            else:
                wait_bytes(dst.at[0:4, :, 0:4 * D_OWN], plane_sem.at[step, k])
            for x in range(4):
                cols = pl.ds(pl.multiple_of((2 * x + core) * D_OWN, D_OWN), D_OWN)
                piece = dst.at[pl.ds(planes[k] * 4, 4), :, cols]
                remote(piece, piece, passed, plane_sem.at[step, 4 + k], sibling).start()
            if k:
                finish(k - 1)
        finish(3)

    gather_team(hid_send, hid_land.at[slot], 0)
    share_down(0)
    wait_bytes(hid_land.at[0:TEAM - 1], recv_sem.at[0])
    for i in range(TEAM):
        x_team[ROWS * i:ROWS * (i + 1), :] = hid_land[i]

    for layer in range(LAYERS):
        base = 8 * layer
        h = norm_rows(x_team[...], norm_attn[layer:layer + 1, :])
        x_block = x_team[:, own_cols]
        take(layer, 0)
        for c in range(Q_OWN // 256):
            cols = slice(c * 256, (c + 1) * 256)
            q = dot_f32(h, wq_buf[layer, :, cols])
            for i in range(TEAM):
                q_send[layer, i, :, cols] = q[ROWS * i:ROWS * (i + 1), :]
        for i in range(1, TEAM):
            to = lax.rem(slot + i, TEAM)
            remote(q_send.at[layer, to], q_land.at[layer, slot], send_sem.at[base + 1], recv_sem.at[base + 1],
                   mate(i)).start()
        pending.append((q_land.at[layer, 0:TEAM - 1], send_sem.at[base + 1]))
        q_land[layer, slot] = q_send[layer, slot]
        wait_bytes(q_land.at[layer, 0:TEAM - 1], recv_sem.at[base + 1])
        for pair, at, sender, col, width in q_segments():
            for r in range(ROWS):
                q_pairs[r, pair:pair + 1, at:at + width] = q_land[layer, sender, r:r + 1, col:col + width]

        take(layer, 1)
        lane = lax.broadcasted_iota(jnp.int32, (16, WIDE), 1)
        key_pos = lax.broadcasted_iota(jnp.int32, (32, SEQ), 1)
        for r in range(ROWS):
            q_even = jnp.where(lane < KV, q_pairs[r, :, 0:WIDE], 0.0).astype(BF16)
            q_odd = jnp.where(lane >= SHIFT, q_pairs[r, :, PAIR - WIDE:PAIR], 0.0).astype(BF16)
            scores = jnp.concatenate([dot_f32(q_even, kv_buf[layer, r, SHIFT:SHIFT + WIDE, :]),
                                      dot_f32(q_odd, kv_buf[layer, r, 0:WIDE, :])], axis=0) * QK_SCALE
            scores = jnp.where(key_pos < lengths[r], scores, -1e30)
            weights = jnp.exp(scores - jnp.max(scores, axis=-1, keepdims=True))
            probs = (weights / jnp.sum(weights, axis=-1, keepdims=True)).astype(BF16)
            context = dot_f32(probs, kv_buf[layer, r, SHIFT:SHIFT + LATENT, :], ((1,), (1,))).astype(BF16)
            o_send[layer, r] = dot_f32(pack[...], context).astype(BF16)
            gather_team(o_send.at[layer, r], o_land.at[layer, slot, r], base + 2)
            o_land[layer, slot, r] = o_send[layer, r]
        wait_bytes(o_land.at[layer, 0:TEAM - 1], recv_sem.at[base + 2])

        o_heads[...] = dot_f32(spread[...], o_land[layer].reshape(TEAM_ROWS * O_ROWS, LATENT)).astype(BF16)
        take(layer, 2)

        heads = jnp.concatenate([o_heads[i * TEAM_ROWS:(i + 1) * TEAM_ROWS, :] for i in range(HEADS)], axis=1)
        delta = dot_f32(heads, wo_buf[layer])
        x_block = (x_block + delta).astype(BF16)
        if layer == 0:
            pl.semaphore_wait(entry_sem, TEAM - 1)
        gather_all(x_block, layer, norm_ffn[layer:layer + 1, :])

        take(layer, 3)
        take(layer, 4)
        gate_up = dot_f32(wgu_buf[layer], g_buf[...], ((1,), (1,)))
        act = (jax.nn.silu(gate_up[0:F_OWN]) * gate_up[F_OWN:]).astype(BF16)
        own_hidden = a_all.at[layer, pl.ds(pl.multiple_of(slot * F_OWN, 16), F_OWN)]
        own_hidden[...] = act
        gather_team(own_hidden, own_hidden, base + 3)
        wait_bytes(a_all.at[layer, 0:F_TEAM - F_OWN], recv_sem.at[base + 3])
        take(layer, 5)
        wait_bytes(wd_buf.at[layer, 0:F_TEAM - F_OWN], down_recv.at[layer])
        part[layer] = dot_f32(a_all[layer], wd_buf[layer], ((0,), (0,))).reshape(TEAMS, TEAM_ROWS, D_OWN)

        def scatter(i, carry):
            to = lax.rem(team + i, TEAMS)
            remote(part.at[layer, to], land.at[layer, team], send_sem.at[base + 4], recv_sem.at[base + 4],
                   to * TEAM + slot).start()
            return carry

        lax.fori_loop(1, TEAMS, scatter, 0)
        pending.append((land.at[layer, 0:TEAMS - 1], send_sem.at[base + 4]))
        if layer + 1 < LAYERS:
            share_down(layer + 1)
        land[layer, team] = part[layer, team]
        wait_bytes(land.at[layer, 0:TEAMS - 1], recv_sem.at[base + 4])
        total = land[layer, 0]
        for i in range(1, TEAMS):
            total = total + land[layer, i]
        x_block = (x_block.astype(F32) + total).astype(BF16)

        if layer == 0:
            own_block = xb_team.at[:, own_cols]
            own_block[...] = x_block
            gather_team(own_block, own_block, 5)
            wait_bytes(xb_team.at[:, 0:D - D_OWN], recv_sem.at[5])
            x_team[...] = xb_team[...].astype(F32)
        else:
            gather_all(x_block, LAYERS, norm_final[...])

    head_load.wait()
    copies = []
    for i, first in enumerate(range(0, VOCAB_OWN, HEAD_CHUNK)):
        size = min(HEAD_CHUNK, VOCAB_OWN - first)
        logits[first:first + size, :] = dot_f32(head_buf[first:first + size, :], g_buf[...], ((1,), (1,)))
        copies.append(pltpu.make_async_copy(logits.at[first:first + size], out.at[first:first + size], out_sem.at[i]))
        copies[-1].start()
    for copy in copies:
        copy.wait()
    for ref, sem in pending:
        wait_bytes(ref, sem)


def make_selectors(pack, spread):
    row = lax.broadcasted_iota(jnp.int32, pack.shape, 0)
    col = lax.broadcasted_iota(jnp.int32, pack.shape, 1)
    hit = (col == (row & 1) * 16 + (row >> 1)) & (row < HEADS)
    pack[...] = jnp.where(hit, 1.0, 0.0).astype(BF16)
    shape = (TEAM_ROWS, TEAM_ROWS * O_ROWS)
    row = lax.broadcasted_iota(jnp.int32, shape, 0)
    col = lax.broadcasted_iota(jnp.int32, shape, 1)
    head = col - row * O_ROWS
    for i in range(HEADS):
        spread[i * TEAM_ROWS:(i + 1) * TEAM_ROWS, :] = jnp.where(head == i, 1.0, 0.0).astype(BF16)


def decode(hidden, lengths, kv_cache, norm_attn, w_q, w_o, norm_ffn, w_gate, w_up, w_down, norm_final, w_head):
    vmem = pl.BlockSpec(memory_space=pltpu.VMEM)
    smem = pl.BlockSpec(memory_space=pltpu.SMEM)
    hbm = pl.BlockSpec(memory_space=pl.ANY)
    dma = pltpu.SemaphoreType.DMA
    return pl.pallas_call(
        decode_kernel,
        out_shape=jax.ShapeDtypeStruct((VOCAB_OWN, ALL_ROWS), F32),
        in_specs=[vmem, smem, hbm, vmem, hbm, hbm, vmem, hbm, hbm, hbm, vmem, hbm],
        out_specs=hbm,
        scratch_shapes=[
            pltpu.VMEM((VOCAB_OWN, D), BF16),
            pltpu.VMEM((VOCAB_OWN, ALL_ROWS), F32),
            pltpu.VMEM((O_ROWS, 32), BF16),
            pltpu.VMEM((HEADS * TEAM_ROWS, TEAM_ROWS * O_ROWS), BF16),
            pltpu.VMEM((ROWS, D), F32),
            pltpu.VMEM((TEAM, ROWS, D), F32),
            pltpu.VMEM((TEAM_ROWS, D), F32),
            pltpu.VMEM((TEAM_ROWS, D), BF16),
            pltpu.VMEM((LAYERS, D, Q_OWN), BF16),
            pltpu.VMEM((LAYERS, ROWS, KV + 2 * SHIFT, SEQ), BF16),
            pltpu.VMEM((LAYERS, HEADS * LATENT, D_OWN), BF16),
            pltpu.VMEM((LAYERS, 2 * F_OWN, D), BF16),
            pltpu.VMEM((LAYERS, F_TEAM, D_OWN), BF16),
            pltpu.VMEM((LAYERS, TEAM, ROWS, Q_OWN), F32),
            pltpu.VMEM((LAYERS, TEAM, ROWS, Q_OWN), F32),
            pltpu.VMEM((ROWS, 16, PAIR), F32),
            pltpu.VMEM((LAYERS, ROWS, O_ROWS, LATENT), BF16),
            pltpu.VMEM((LAYERS, TEAM, ROWS, O_ROWS, LATENT), BF16),
            pltpu.VMEM((HEADS * TEAM_ROWS, LATENT), BF16),
            pltpu.VMEM((LAYERS + 1, TEAMS, TEAM_ROWS, D), BF16),
            pltpu.VMEM((ALL_ROWS, D), BF16),
            pltpu.VMEM((LAYERS, F_TEAM, ALL_ROWS), BF16),
            pltpu.VMEM((LAYERS, TEAMS, TEAM_ROWS, D_OWN), F32),
            pltpu.VMEM((LAYERS, TEAMS, TEAM_ROWS, D_OWN), F32),
            dma((LAYERS, 6)),
            pltpu.SemaphoreType.REGULAR,
            dma((22,)),
            dma((22,)),
            dma((LAYERS + 1, 8)),
            dma((LAYERS,)),
            dma((LAYERS,)),
            dma,
            dma((-(-VOCAB_OWN // HEAD_CHUNK),)),
        ],
        compiler_params=pltpu.CompilerParams(collective_id=0, has_side_effects=True, vmem_limit_bytes=60 * 1024 * 1024),
        name='decode',
    )(hidden, lengths, kv_cache, norm_attn, w_q, w_o, norm_ffn, w_gate, w_up, w_down, norm_final, w_head)


def solution(mesh):
    row_axes = ('rep', 'dp')
    specs_in = (P(row_axes, None), P(row_axes), P(None, row_axes, None, None), P(), P(), P(), P(),
                P(None, None, 'dp'), P(None, None, 'dp'), P(None, 'dp', None), P(), P(None, 'dp'))

    def device_step(hidden, lengths, kv_cache, norm_attn, w_q, w_o, norm_ffn, w_gate, w_up, w_down, norm_final, w_head):
        logits = decode(hidden, lengths, jnp.swapaxes(kv_cache, 2, 3), norm_attn, w_q, w_o, norm_ffn,
                        jnp.swapaxes(w_gate, 1, 2), jnp.swapaxes(w_up, 1, 2), w_down, norm_final.reshape(1, -1),
                        jnp.swapaxes(w_head, 0, 1))
        return jnp.swapaxes(logits, 0, 1)

    return jax.shard_map(device_step, mesh=mesh, in_specs=specs_in, out_specs=P('rep', 'dp'), check_vma=False)
```

```python
import jax
import jax.numpy as jnp
from jax import lax
from jax.experimental import pallas as pl
from jax.experimental.pallas import tpu as pltpu
from jax.sharding import PartitionSpec as P

MESH = pl.DeviceIdType.MESH
QK_SCALE = 192 ** -0.5
NORM_EPS = 1e-6

LAYERS = 2
ROWS = 2
TEAM = 8
TEAMS = 16
TEAM_ROWS = ROWS * TEAM
ALL_ROWS = TEAM_ROWS * TEAMS
HALF = ALL_ROWS // 2
D = 2048
D_OWN = D // TEAM
HEADS = 20
LATENT = 512
KV = 576
SEQ = 512
Q_COLS = HEADS * KV
Q_OWN = 1536
Q_LAST = Q_COLS - Q_OWN
PAIR = 2 * KV
PAIRS = HEADS // 2
SHIFT = 64
WIDE = KV + SHIFT
O_ROWS = 24
F_OWN = 80
F_TEAM = F_OWN * TEAM
VOCAB_OWN = 1210
HEAD_CHUNK = 304
F32 = jnp.float32
BF16 = jnp.bfloat16


def norm_rows(x, gain):
    inv_rms = lax.rsqrt(jnp.mean(x * x, axis=-1, keepdims=True) + NORM_EPS)
    return (x * inv_rms * gain).astype(BF16)


def dot_f32(a, b, contract=((1,), (0,))):
    return lax.dot_general(a, b, (contract, ((), ())), preferred_element_type=F32)


def wait_bytes(ref, sem):
    pltpu.make_async_copy(ref, ref, sem).wait()


def q_segments():
    pieces = []
    for pair in range(PAIRS):
        at, end = pair * PAIR, (pair + 1) * PAIR
        while at < end:
            sender = at // Q_OWN
            first = min(sender * Q_OWN, Q_LAST)
            stop = min(end, (sender + 1) * Q_OWN, Q_COLS)
            pieces.append((pair, at - pair * PAIR, sender, at - first, stop - at))
            at = stop
    return pieces


def decode_kernel(hidden, lengths, kv_cache, norm_attn, w_q, w_o, norm_ffn, w_gate, w_up, w_down, norm_final, w_head,
                  out, head_buf, logits, pack, spread, hid_land, x_team, xb_team, wq_buf, kv_buf, wo_buf, wgu_buf, wd_buf,
                  q_send, q_land, q_pairs, o_send, o_land, o_heads, x_all, g_buf, a_all, part, land,
                  load_sem, entry_sem, send_sem, recv_sem, plane_sem, down_send, down_recv, near_sem, head_sem, out_sem):
    me = lax.axis_index('dp')
    team, slot = me // TEAM, lax.rem(me, TEAM)
    plane, core = team // 4, lax.rem(me, 2)
    sibling = me + 1 - 2 * core
    own_cols = pl.ds(pl.multiple_of(slot * D_OWN, D_OWN), D_OWN)
    q_start = pl.multiple_of(jnp.minimum(slot * Q_OWN, Q_LAST), 128)

    pending = []

    def take(layer, i):
        loads[layer][i].wait()

    def mate(i):
        return team * TEAM + lax.rem(slot + i, TEAM)

    def remote(src, dst, ssem, rsem, device):
        return pltpu.make_async_remote_copy(src, dst, ssem, rsem, device_id={'dp': device}, device_id_type=MESH)

    barrier = pltpu.get_barrier_semaphore()
    for i in range(1, TEAM):
        pl.semaphore_signal(barrier, inc=1, device_id={'dp': mate(i)}, device_id_type=MESH)

    def greet(i, carry):
        pl.semaphore_signal(barrier, inc=1, device_id={'dp': lax.rem(me + i * TEAM, TEAM * TEAMS)}, device_id_type=MESH)
        return carry

    lax.fori_loop(1, TEAMS, greet, 0)

    loads = []
    for layer in range(LAYERS):
        batch = [
            (w_q.at[layer, :, pl.ds(q_start, Q_OWN)], wq_buf.at[layer]),
            (kv_cache.at[layer], kv_buf.at[layer, :, pl.ds(SHIFT, KV)]),
            (w_o.at[layer, :, own_cols], wo_buf.at[layer]),
            (w_gate.at[layer], wgu_buf.at[layer, pl.ds(0, F_OWN)]),
            (w_up.at[layer], wgu_buf.at[layer, pl.ds(F_OWN, F_OWN)]),
            (w_down.at[layer, :, own_cols], wd_buf.at[layer, pl.ds(pl.multiple_of(slot * F_OWN, 16), F_OWN)]),
        ]
        loads.append([pltpu.make_async_copy(src, dst, load_sem.at[layer, i]) for i, (src, dst) in enumerate(batch)])
    for batch in loads:
        for copy in batch:
            copy.start()
    head_load = pltpu.make_async_copy(w_head, head_buf, head_sem)
    head_load.start()

    for layer in range(LAYERS):
        for r in range(ROWS):
            kv_buf[layer, r, 0:SHIFT, :] = jnp.zeros((SHIFT, SEQ), BF16)
            kv_buf[layer, r, SHIFT + KV:, :] = jnp.zeros((SHIFT, SEQ), BF16)
    q_pairs[...] = jnp.zeros_like(q_pairs)
    make_selectors(pack, spread)
    hid_land[slot] = hidden[...]

    pl.semaphore_wait(barrier, TEAM - 1 + TEAMS - 1)
    for i in range(1, TEAM):
        pl.semaphore_signal(entry_sem, inc=1, device_id={'dp': mate(i)}, device_id_type=MESH)

    def gather_team(src, dst, sem):
        for i in range(1, TEAM):
            remote(src, dst, send_sem.at[sem], recv_sem.at[sem], mate(i)).start()
            pending.append((src, send_sem.at[sem]))

    def share_down(layer):
        for i in range(1, TEAM):
            to = lax.rem(slot + i, TEAM)
            remote(w_down.at[layer, :, pl.ds(pl.multiple_of(to * D_OWN, D_OWN), D_OWN)],
                   wd_buf.at[layer, pl.ds(pl.multiple_of(slot * F_OWN, 16), F_OWN)],
                   down_send.at[layer], down_recv.at[layer], mate(i)).start()
        pending.append((wd_buf.at[layer, 0:F_TEAM - F_OWN], down_send.at[layer]))

    def gather_all(block, step, gain, use_half):
        dst = x_all.at[step]
        mine = dst.at[team, :, own_cols]
        mine[...] = block
        direct, passed = send_sem.at[16 + 2 * step], send_sem.at[17 + 2 * step]
        planes = (plane, plane + 1 - 2 * lax.rem(plane, 2), 3 - plane, lax.rem(plane + 2, 4))
        for k in (3, 2, 1, 0):

            def send(i, carry, k=k):
                spot = lax.rem(lax.rem(me, 32) // 2 + 24 - i, 16)
                remote(mine, mine, direct, plane_sem.at[step, k], planes[k] * 32 + spot * 2 + core).start()
                return carry

            def send_near(i, carry, k=k):
                spot = lax.rem(lax.rem(me, 32) // 2 + i, 16)
                remote(mine, mine, direct, plane_sem.at[step, k], planes[k] * 32 + spot * 2 + core).start()
                return carry

            if k:
                lax.fori_loop(0, 16, send, 0)
            else:
                lax.fori_loop(1, 16, send_near, 0)
        pending.append((dst.at[0:7], direct))
        pending.append((dst.at[0, :, 0:7 * D_OWN], direct))
        pending.append((dst.at[0:8], passed))

        def finish(k):
            wait_bytes(dst.at[0:4, :, 0:4 * D_OWN], plane_sem.at[step, 4 + k])

            def chunk(i, carry):
                row = planes[k] * 4 + i
                g_buf[pl.ds(pl.multiple_of(row * TEAM_ROWS, TEAM_ROWS), TEAM_ROWS), :] = norm_rows(
                    dst[row].astype(F32), gain)
                return carry

            lax.fori_loop(0, 4, chunk, 0)

        for half in range(2):
            for k in (2 * half, 2 * half + 1):
                if k == 0:
                    wait_bytes(dst.at[0:3, :, 0:5 * D_OWN], plane_sem.at[step, k])
                else:
                    wait_bytes(dst.at[0:4, :, 0:4 * D_OWN], plane_sem.at[step, k])
                for x in range(4):
                    cols = pl.ds(pl.multiple_of((2 * x + core) * D_OWN, D_OWN), D_OWN)
                    piece = dst.at[pl.ds(planes[k] * 4, 4), :, cols]
                    remote(piece, piece, passed, plane_sem.at[step, 4 + k], sibling).start()
            finish(2 * half)
            finish(2 * half + 1)
            use_half(half)

    gather_team(hidden, hid_land.at[slot], 0)
    share_down(0)
    wait_bytes(hid_land.at[0:TEAM - 1], recv_sem.at[0])
    for i in range(TEAM):
        x_team[ROWS * i:ROWS * (i + 1), :] = hid_land[i].astype(F32)

    for layer in range(LAYERS):
        base = 8 * layer
        h = norm_rows(x_team[...], norm_attn[layer:layer + 1, :])
        x_block = x_team[:, own_cols]
        take(layer, 0)
        for c in range(Q_OWN // 256):
            cols = slice(c * 256, (c + 1) * 256)
            q = dot_f32(h, wq_buf[layer, :, cols])
            for i in range(TEAM):
                q_send[layer, i, :, cols] = q[ROWS * i:ROWS * (i + 1), :].astype(BF16)
        for i in range(1, TEAM):
            to = lax.rem(slot + i, TEAM)
            remote(q_send.at[layer, to], q_land.at[layer, slot], send_sem.at[base + 1], recv_sem.at[base + 1],
                   mate(i)).start()
        pending.append((q_land.at[layer, 0:TEAM - 1], send_sem.at[base + 1]))
        q_land[layer, slot] = q_send[layer, slot]
        wait_bytes(q_land.at[layer, 0:TEAM - 1], recv_sem.at[base + 1])
        for pair, at, sender, col, width in q_segments():
            piece = q_land[layer, sender, :, col:col + width].astype(F32)
            for r in range(ROWS):
                q_pairs[r, pair:pair + 1, at:at + width] = piece[r:r + 1]

        take(layer, 1)
        lane = lax.broadcasted_iota(jnp.int32, (16, WIDE), 1)
        key_pos = lax.broadcasted_iota(jnp.int32, (32, SEQ), 1)
        for r in range(ROWS):
            q_even = jnp.where(lane < KV, q_pairs[r, :, 0:WIDE], 0.0).astype(BF16)
            q_odd = jnp.where(lane >= SHIFT, q_pairs[r, :, PAIR - WIDE:PAIR], 0.0).astype(BF16)
            scores = jnp.concatenate([dot_f32(q_even, kv_buf[layer, r, SHIFT:SHIFT + WIDE, :]),
                                      dot_f32(q_odd, kv_buf[layer, r, 0:WIDE, :])], axis=0) * QK_SCALE
            scores = jnp.where(key_pos < lengths[r], scores, -1e30)
            weights = jnp.exp(scores - jnp.max(scores, axis=-1, keepdims=True))
            probs = (weights / jnp.sum(weights, axis=-1, keepdims=True)).astype(BF16)
            context = dot_f32(probs, kv_buf[layer, r, SHIFT:SHIFT + LATENT, :], ((1,), (1,))).astype(BF16)
            o_send[layer, r] = dot_f32(pack[...], context).astype(BF16)
            block, dst = o_send.at[layer, r], o_land.at[layer, slot, r]
            osem, orecv = send_sem.at[base + 2], recv_sem.at[base + 2]
            for i in (4, 4 + 1 - 2 * core):
                remote(block, dst, osem, orecv, mate(i)).start()
            remote(block, dst, osem, near_sem.at[layer, r, 0], mate(2)).start()
            remote(block, dst, osem, near_sem.at[layer, r, 1], mate(TEAM - 2)).start()
            remote(block, dst, osem, orecv, sibling).start()
            o_land[layer, slot, r] = o_send[layer, r]
            pending.extend([(block, osem)] * (TEAM - 1))
        for r in range(ROWS):
            for side, i in enumerate((TEAM - 2, 2)):
                piece = o_land.at[layer, lax.rem(slot + i, TEAM), r]
                wait_bytes(piece, near_sem.at[layer, r, side])
                remote(piece, piece, send_sem.at[base + 2], recv_sem.at[base + 2], sibling).start()
        wait_bytes(o_land.at[layer, 0:TEAM - 3], recv_sem.at[base + 2])

        o_heads[...] = dot_f32(spread[...], o_land[layer].reshape(TEAM_ROWS * O_ROWS, LATENT)).astype(BF16)
        take(layer, 2)

        heads = jnp.concatenate([o_heads[i * TEAM_ROWS:(i + 1) * TEAM_ROWS, :] for i in range(HEADS)], axis=1)
        delta = dot_f32(heads, wo_buf[layer])
        x_block = (x_block + delta).astype(BF16)
        if layer == 0:
            pl.semaphore_wait(entry_sem, TEAM - 1)
        own_pair = plane // 2
        pairs = (own_pair, 1 - own_pair)

        def half_rows(half):
            return pl.ds(pl.multiple_of(pairs[half] * HALF, HALF), HALF)

        def activate(half, layer=layer, base=base):
            if half == 0:
                take(layer, 3)
                take(layer, 4)
            gate_up = dot_f32(wgu_buf[layer], g_buf[half_rows(half), :], ((1,), (1,)))
            act = (jax.nn.silu(gate_up[0:F_OWN]) * gate_up[F_OWN:]).astype(BF16)
            own_hidden = a_all.at[layer, pl.ds(pl.multiple_of(slot * F_OWN, 16), F_OWN), half_rows(half)]
            own_hidden[...] = act
            gather_team(own_hidden, own_hidden, base + 3 + 2 * half)

        gather_all(x_block, layer, norm_ffn[layer:layer + 1, :], activate)
        for half in range(2):
            wait_bytes(a_all.at[layer, 0:F_TEAM - F_OWN, 0:HALF], recv_sem.at[base + 3 + 2 * half])
            if half == 0:
                take(layer, 5)
                wait_bytes(wd_buf.at[layer, 0:F_TEAM - F_OWN], down_recv.at[layer])
            first = pairs[half] * (TEAMS // 2)
            part[layer, pl.ds(first, TEAMS // 2)] = dot_f32(
                a_all[layer, :, half_rows(half)], wd_buf[layer], ((0,), (0,))).reshape(TEAMS // 2, TEAM_ROWS, D_OWN)

            def scatter(i, carry, first=first):
                to = first + lax.rem(lax.rem(team, TEAMS // 2) + i, TEAMS // 2)
                remote(part.at[layer, to], land.at[layer, team], send_sem.at[base + 4], recv_sem.at[base + 4],
                       to * TEAM + slot).start()
                return carry

            lax.fori_loop(1 - half, TEAMS // 2, scatter, 0)
        pending.append((land.at[layer, 0:TEAMS - 1], send_sem.at[base + 4]))
        if layer + 1 < LAYERS:
            share_down(layer + 1)
        land[layer, team] = part[layer, team]
        wait_bytes(land.at[layer, 0:TEAMS - 1], recv_sem.at[base + 4])
        total = land[layer, 0]
        for i in range(1, TEAMS):
            total = total + land[layer, i]
        x_block = (x_block.astype(F32) + total).astype(BF16)

        if layer == 0:
            own_block = xb_team.at[:, own_cols]
            own_block[...] = x_block
            gather_team(own_block, own_block, 6)
            wait_bytes(xb_team.at[:, 0:D - D_OWN], recv_sem.at[6])
            x_team[...] = xb_team[...].astype(F32)
        else:
            gather_all(x_block, LAYERS, norm_final[...], lambda half: None)

    head_load.wait()
    copies = []
    for i, first in enumerate(range(0, VOCAB_OWN, HEAD_CHUNK)):
        size = min(HEAD_CHUNK, VOCAB_OWN - first)
        logits[first:first + size, :] = dot_f32(head_buf[first:first + size, :], g_buf[...], ((1,), (1,)))
        copies.append(pltpu.make_async_copy(logits.at[first:first + size], out.at[first:first + size], out_sem.at[i]))
        copies[-1].start()
    for copy in copies:
        copy.wait()
    for ref, sem in pending:
        wait_bytes(ref, sem)


def make_selectors(pack, spread):
    row = lax.broadcasted_iota(jnp.int32, pack.shape, 0)
    col = lax.broadcasted_iota(jnp.int32, pack.shape, 1)
    hit = (col == (row & 1) * 16 + (row >> 1)) & (row < HEADS)
    pack[...] = jnp.where(hit, 1.0, 0.0).astype(BF16)
    shape = (TEAM_ROWS, TEAM_ROWS * O_ROWS)
    row = lax.broadcasted_iota(jnp.int32, shape, 0)
    col = lax.broadcasted_iota(jnp.int32, shape, 1)
    head = col - row * O_ROWS
    for i in range(HEADS):
        spread[i * TEAM_ROWS:(i + 1) * TEAM_ROWS, :] = jnp.where(head == i, 1.0, 0.0).astype(BF16)


def decode(hidden, lengths, kv_cache, norm_attn, w_q, w_o, norm_ffn, w_gate, w_up, w_down, norm_final, w_head):
    vmem = pl.BlockSpec(memory_space=pltpu.VMEM)
    smem = pl.BlockSpec(memory_space=pltpu.SMEM)
    hbm = pl.BlockSpec(memory_space=pl.ANY)
    dma = pltpu.SemaphoreType.DMA
    return pl.pallas_call(
        decode_kernel,
        out_shape=jax.ShapeDtypeStruct((VOCAB_OWN, ALL_ROWS), F32),
        in_specs=[vmem, smem, hbm, vmem, hbm, hbm, vmem, hbm, hbm, hbm, vmem, hbm],
        out_specs=hbm,
        scratch_shapes=[
            pltpu.VMEM((VOCAB_OWN, D), BF16),
            pltpu.VMEM((VOCAB_OWN, ALL_ROWS), F32),
            pltpu.VMEM((O_ROWS, 32), BF16),
            pltpu.VMEM((HEADS * TEAM_ROWS, TEAM_ROWS * O_ROWS), BF16),
            pltpu.VMEM((TEAM, ROWS, D), BF16),
            pltpu.VMEM((TEAM_ROWS, D), F32),
            pltpu.VMEM((TEAM_ROWS, D), BF16),
            pltpu.VMEM((LAYERS, D, Q_OWN), BF16),
            pltpu.VMEM((LAYERS, ROWS, KV + 2 * SHIFT, SEQ), BF16),
            pltpu.VMEM((LAYERS, HEADS * LATENT, D_OWN), BF16),
            pltpu.VMEM((LAYERS, 2 * F_OWN, D), BF16),
            pltpu.VMEM((LAYERS, F_TEAM, D_OWN), BF16),
            pltpu.VMEM((LAYERS, TEAM, ROWS, Q_OWN), BF16),
            pltpu.VMEM((LAYERS, TEAM, ROWS, Q_OWN), BF16),
            pltpu.VMEM((ROWS, 16, PAIR), F32),
            pltpu.VMEM((LAYERS, ROWS, O_ROWS, LATENT), BF16),
            pltpu.VMEM((LAYERS, TEAM, ROWS, O_ROWS, LATENT), BF16),
            pltpu.VMEM((HEADS * TEAM_ROWS, LATENT), BF16),
            pltpu.VMEM((LAYERS + 1, TEAMS, TEAM_ROWS, D), BF16),
            pltpu.VMEM((ALL_ROWS, D), BF16),
            pltpu.VMEM((LAYERS, F_TEAM, ALL_ROWS), BF16),
            pltpu.VMEM((LAYERS, TEAMS, TEAM_ROWS, D_OWN), F32),
            pltpu.VMEM((LAYERS, TEAMS, TEAM_ROWS, D_OWN), F32),
            dma((LAYERS, 6)),
            pltpu.SemaphoreType.REGULAR,
            dma((22,)),
            dma((22,)),
            dma((LAYERS + 1, 8)),
            dma((LAYERS,)),
            dma((LAYERS,)),
            dma((LAYERS, ROWS, 2)),
            dma,
            dma((-(-VOCAB_OWN // HEAD_CHUNK),)),
        ],
        compiler_params=pltpu.CompilerParams(collective_id=0, has_side_effects=True, vmem_limit_bytes=60 * 1024 * 1024),
        name='decode',
    )(hidden, lengths, kv_cache, norm_attn, w_q, w_o, norm_ffn, w_gate, w_up, w_down, norm_final, w_head)


def solution(mesh):
    row_axes = ('rep', 'dp')
    specs_in = (P(row_axes, None), P(row_axes), P(None, row_axes, None, None), P(), P(), P(), P(),
                P(None, None, 'dp'), P(None, None, 'dp'), P(None, 'dp', None), P(), P(None, 'dp'))

    def device_step(hidden, lengths, kv_cache, norm_attn, w_q, w_o, norm_ffn, w_gate, w_up, w_down, norm_final, w_head):
        logits = decode(hidden, lengths, jnp.swapaxes(kv_cache, 2, 3), norm_attn, w_q, w_o, norm_ffn,
                        jnp.swapaxes(w_gate, 1, 2), jnp.swapaxes(w_up, 1, 2), w_down, norm_final.reshape(1, -1),
                        jnp.swapaxes(w_head, 0, 1))
        return jnp.swapaxes(logits, 0, 1)

    return jax.shard_map(device_step, mesh=mesh, in_specs=specs_in, out_specs=P('rep', 'dp'), check_vma=False)
```

```python
import jax
import jax.numpy as jnp
from jax import lax
from jax.experimental import pallas as pl
from jax.experimental.pallas import tpu as pltpu
from jax.sharding import PartitionSpec as P

MESH = pl.DeviceIdType.MESH
QK_SCALE = 192 ** -0.5
NORM_EPS = 1e-6

LAYERS = 2
ROWS = 2
TEAM = 8
TEAMS = 16
TEAM_ROWS = ROWS * TEAM
ALL_ROWS = TEAM_ROWS * TEAMS
HALF = ALL_ROWS // 2
D = 2048
D_OWN = D // TEAM
HEADS = 20
LATENT = 512
KV = 576
SEQ = 512
Q_COLS = HEADS * KV
Q_OWN = 1536
Q_LAST = Q_COLS - Q_OWN
PAIR = 2 * KV
PAIRS = HEADS // 2
SHIFT = 64
WIDE = KV + SHIFT
O_ROWS = 2 * HEADS
O_COLS = LATENT // 2
F_OWN = 80
F_TEAM = F_OWN * TEAM
VOCAB_OWN = 1210
HEAD_CHUNK = 304
F32 = jnp.float32
BF16 = jnp.bfloat16


def norm_rows(x, gain):
    inv_rms = lax.rsqrt(jnp.mean(x * x, axis=-1, keepdims=True) + NORM_EPS)
    return (x * inv_rms * gain).astype(BF16)


def dot_f32(a, b, contract=((1,), (0,))):
    return lax.dot_general(a, b, (contract, ((), ())), preferred_element_type=F32)


def wait_bytes(ref, sem):
    pltpu.make_async_copy(ref, ref, sem).wait()


def q_segments():
    pieces = []
    for pair in range(PAIRS):
        at, end = pair * PAIR, (pair + 1) * PAIR
        while at < end:
            sender = at // Q_OWN
            first = min(sender * Q_OWN, Q_LAST)
            stop = min(end, (sender + 1) * Q_OWN, Q_COLS)
            pieces.append((pair, at - pair * PAIR, sender, at - first, stop - at))
            at = stop
    return pieces


def decode_kernel(hidden_in, lengths_in, kv_cache, norm_attn_in, w_q, w_o, norm_ffn_in, w_gate, w_up, w_down, norm_final_in, w_head,
                  out, hidden, lengths, norm_attn, norm_ffn, norm_final, head_buf, logits, pack, spread, hid_land, x_team, xb_team, wq_buf, kv_buf, wo_buf, wgu_buf, wd_buf,
                  q_send, q_land, q_pairs, o_send, o_land, o_heads, x_all, g_buf, a_all, part, land,
                  load_sem, entry_sem, send_sem, recv_sem, plane_sem, down_send, down_recv, near_sem, head_sem, out_sem, small_sem):
    me = lax.axis_index('dp')
    team, slot = me // TEAM, lax.rem(me, TEAM)
    plane, core = team // 4, lax.rem(me, 2)
    sibling = me + 1 - 2 * core
    own_cols = pl.ds(pl.multiple_of(slot * D_OWN, D_OWN), D_OWN)
    q_start = pl.multiple_of(jnp.minimum(slot * Q_OWN, Q_LAST), 128)

    pending = []

    def take(layer, i):
        loads[layer][i].wait()

    def mate(i):
        return team * TEAM + lax.rem(slot + i, TEAM)

    def remote(src, dst, ssem, rsem, device):
        return pltpu.make_async_remote_copy(src, dst, ssem, rsem, device_id={'dp': device}, device_id_type=MESH)

    barrier = pltpu.get_barrier_semaphore()
    for i in range(1, TEAM):
        pl.semaphore_signal(barrier, inc=1, device_id={'dp': mate(i)}, device_id_type=MESH)

    def greet(i, carry):
        pl.semaphore_signal(barrier, inc=1, device_id={'dp': lax.rem(me + i * TEAM, TEAM * TEAMS)}, device_id_type=MESH)
        return carry

    lax.fori_loop(1, TEAMS, greet, 0)

    smalls = [pltpu.make_async_copy(src, dst, small_sem.at[i]) for i, (src, dst) in enumerate((
        (hidden_in, hidden), (norm_attn_in, norm_attn), (lengths_in, lengths), (norm_ffn_in, norm_ffn),
        (norm_final_in, norm_final)))]
    for copy in smalls:
        copy.start()

    loads = []
    for layer in range(LAYERS):
        batch = [
            (w_q.at[layer, :, pl.ds(q_start, Q_OWN)], wq_buf.at[layer]),
            (kv_cache.at[layer], kv_buf.at[layer, :, pl.ds(SHIFT, KV)]),
            (w_o.at[layer, :, own_cols], wo_buf.at[layer]),
            (w_gate.at[layer], wgu_buf.at[layer, pl.ds(0, F_OWN)]),
            (w_up.at[layer], wgu_buf.at[layer, pl.ds(F_OWN, F_OWN)]),
            (w_down.at[layer, :, own_cols], wd_buf.at[layer, pl.ds(pl.multiple_of(slot * F_OWN, 16), F_OWN)]),
        ]
        loads.append([pltpu.make_async_copy(src, dst, load_sem.at[layer, i]) for i, (src, dst) in enumerate(batch)])
    for batch in loads:
        for copy in batch:
            copy.start()
    head_load = pltpu.make_async_copy(w_head, head_buf, head_sem)
    head_load.start()

    for layer in range(LAYERS):
        for r in range(ROWS):
            kv_buf[layer, r, 0:SHIFT, :] = jnp.zeros((SHIFT, SEQ), BF16)
            kv_buf[layer, r, SHIFT + KV:, :] = jnp.zeros((SHIFT, SEQ), BF16)
    q_pairs[...] = jnp.zeros_like(q_pairs)
    make_selectors(pack, spread)
    for copy in smalls:
        copy.wait()
    hid_land[slot] = hidden[...]

    pl.semaphore_wait(barrier, TEAM - 1 + TEAMS - 1)
    for i in range(1, TEAM):
        pl.semaphore_signal(entry_sem, inc=1, device_id={'dp': mate(i)}, device_id_type=MESH)

    def gather_team(src, dst, sem):
        for i in range(1, TEAM):
            remote(src, dst, send_sem.at[sem], recv_sem.at[sem], mate(i)).start()
            pending.append((src, send_sem.at[sem]))

    def share_down(layer):
        for i in range(1, TEAM):
            to = lax.rem(slot + i, TEAM)
            remote(w_down.at[layer, :, pl.ds(pl.multiple_of(to * D_OWN, D_OWN), D_OWN)],
                   wd_buf.at[layer, pl.ds(pl.multiple_of(slot * F_OWN, 16), F_OWN)],
                   down_send.at[layer], down_recv.at[layer], mate(i)).start()
        pending.append((wd_buf.at[layer, 0:F_TEAM - F_OWN], down_send.at[layer]))

    def gather_all(block, step, gain, use_half):
        dst = x_all.at[step]
        mine = dst.at[team, :, own_cols]
        mine[...] = block
        direct, passed = send_sem.at[16 + 2 * step], send_sem.at[17 + 2 * step]
        planes = (plane, plane + 1 - 2 * lax.rem(plane, 2), 3 - plane, lax.rem(plane + 2, 4))
        for k in (1, 0, 3, 2) if step < LAYERS else (3, 2, 1, 0):

            def send(i, carry, k=k):
                spot = lax.rem(lax.rem(me, 32) // 2 + 24 - i, 16)
                remote(mine, mine, direct, plane_sem.at[step, k], planes[k] * 32 + spot * 2 + core).start()
                return carry

            def send_near(i, carry, k=k):
                spot = lax.rem(lax.rem(me, 32) // 2 + i, 16)
                remote(mine, mine, direct, plane_sem.at[step, k], planes[k] * 32 + spot * 2 + core).start()
                return carry

            if k:
                lax.fori_loop(0, 16, send, 0)
            else:
                lax.fori_loop(1, 16, send_near, 0)
        pending.append((dst.at[0:7], direct))
        pending.append((dst.at[0, :, 0:7 * D_OWN], direct))
        pending.append((dst.at[0:8], passed))

        def finish(k):
            wait_bytes(dst.at[0:4, :, 0:4 * D_OWN], plane_sem.at[step, 4 + k])

            def chunk(i, carry):
                row = planes[k] * 4 + i
                g_buf[pl.ds(pl.multiple_of(row * TEAM_ROWS, TEAM_ROWS), TEAM_ROWS), :] = norm_rows(
                    dst[row].astype(F32), gain)
                return carry

            lax.fori_loop(0, 4, chunk, 0)

        for half in range(2):
            for k in (2 * half, 2 * half + 1):
                if k == 0:
                    wait_bytes(dst.at[0:3, :, 0:5 * D_OWN], plane_sem.at[step, k])
                else:
                    wait_bytes(dst.at[0:4, :, 0:4 * D_OWN], plane_sem.at[step, k])
                for x in range(4):
                    cols = pl.ds(pl.multiple_of((2 * x + core) * D_OWN, D_OWN), D_OWN)
                    piece = dst.at[pl.ds(planes[k] * 4, 4), :, cols]
                    remote(piece, piece, passed, plane_sem.at[step, 4 + k], sibling).start()
            finish(2 * half)
            finish(2 * half + 1)
            use_half(half)

    gather_team(hidden, hid_land.at[slot], 0)
    share_down(0)
    wait_bytes(hid_land.at[0:TEAM - 1], recv_sem.at[0])
    for i in range(TEAM):
        x_team[ROWS * i:ROWS * (i + 1), :] = hid_land[i].astype(F32)

    for layer in range(LAYERS):
        base = 8 * layer
        h = norm_rows(x_team[...], norm_attn[layer:layer + 1, :])
        x_block = x_team[:, own_cols]
        take(layer, 0)
        for c in range(Q_OWN // 256):
            cols = slice(c * 256, (c + 1) * 256)
            q = dot_f32(h, wq_buf[layer, :, cols])
            for i in range(TEAM):
                q_send[layer, i, :, cols] = q[ROWS * i:ROWS * (i + 1), :].astype(BF16)
        for i in range(1, TEAM):
            to = lax.rem(slot + i, TEAM)
            remote(q_send.at[layer, to], q_land.at[layer, slot], send_sem.at[base + 1], recv_sem.at[base + 1],
                   mate(i)).start()
        pending.append((q_land.at[layer, 0:TEAM - 1], send_sem.at[base + 1]))
        q_land[layer, slot] = q_send[layer, slot]
        wait_bytes(q_land.at[layer, 0:TEAM - 1], recv_sem.at[base + 1])
        for pair, at, sender, col, width in q_segments():
            piece = q_land[layer, sender, :, col:col + width].astype(F32)
            for r in range(ROWS):
                q_pairs[r, pair:pair + 1, at:at + width] = piece[r:r + 1]

        take(layer, 1)
        lane = lax.broadcasted_iota(jnp.int32, (16, WIDE), 1)
        key_pos = lax.broadcasted_iota(jnp.int32, (32, SEQ), 1)
        for r in range(ROWS):
            q_even = jnp.where(lane < KV, q_pairs[r, :, 0:WIDE], 0.0).astype(BF16)
            q_odd = jnp.where(lane >= SHIFT, q_pairs[r, :, PAIR - WIDE:PAIR], 0.0).astype(BF16)
            scores = jnp.concatenate([dot_f32(q_even, kv_buf[layer, r, SHIFT:SHIFT + WIDE, :]),
                                      dot_f32(q_odd, kv_buf[layer, r, 0:WIDE, :])], axis=0) * QK_SCALE
            scores = jnp.where(key_pos < lengths[r], scores, -1e30)
            weights = jnp.exp(scores - jnp.max(scores, axis=-1, keepdims=True))
            probs = (weights / jnp.sum(weights, axis=-1, keepdims=True)).astype(BF16)
            context = dot_f32(probs, kv_buf[layer, r, SHIFT:SHIFT + LATENT, :], ((1,), (1,))).astype(BF16)
            halves = jnp.concatenate([context[:, :O_COLS], context[:, O_COLS:]], axis=0)
            o_send[layer, r] = dot_f32(pack[...], halves).astype(BF16)
            block, dst = o_send.at[layer, r], o_land.at[layer, slot, r]
            osem, orecv = send_sem.at[base + 2], recv_sem.at[base + 2]
            for i in (4, 4 + 1 - 2 * core):
                remote(block, dst, osem, orecv, mate(i)).start()
            remote(block, dst, osem, near_sem.at[layer, r, 0], mate(2)).start()
            remote(block, dst, osem, near_sem.at[layer, r, 1], mate(TEAM - 2)).start()
            remote(block, dst, osem, orecv, sibling).start()
            o_land[layer, slot, r] = o_send[layer, r]
            pending.extend([(block, osem)] * (TEAM - 1))
        for r in range(ROWS):
            for side, i in enumerate((TEAM - 2, 2)):
                piece = o_land.at[layer, lax.rem(slot + i, TEAM), r]
                wait_bytes(piece, near_sem.at[layer, r, side])
                remote(piece, piece, send_sem.at[base + 2], recv_sem.at[base + 2], sibling).start()
        wait_bytes(o_land.at[layer, 0:TEAM - 3], recv_sem.at[base + 2])

        o_heads[...] = dot_f32(spread[...], o_land[layer].reshape(TEAM_ROWS * O_ROWS, O_COLS)).astype(BF16)
        take(layer, 2)

        heads = jnp.concatenate([o_heads[i * TEAM_ROWS:(i + 1) * TEAM_ROWS, :] for i in range(O_ROWS)], axis=1)
        delta = dot_f32(heads, wo_buf[layer])
        x_block = (x_block + delta).astype(BF16)
        if layer == 0:
            pl.semaphore_wait(entry_sem, TEAM - 1)
        own_pair = plane // 2
        pairs = (own_pair, 1 - own_pair)

        def half_rows(half):
            return pl.ds(pl.multiple_of(pairs[half] * HALF, HALF), HALF)

        def activate(half, layer=layer, base=base):
            if half == 0:
                take(layer, 3)
                take(layer, 4)
            gate_up = dot_f32(wgu_buf[layer], g_buf[half_rows(half), :], ((1,), (1,)))
            act = (jax.nn.silu(gate_up[0:F_OWN]) * gate_up[F_OWN:]).astype(BF16)
            own_hidden = a_all.at[layer, pl.ds(pl.multiple_of(slot * F_OWN, 16), F_OWN), half_rows(half)]
            own_hidden[...] = act
            gather_team(own_hidden, own_hidden, base + 3 + 2 * half)

        gather_all(x_block, layer, norm_ffn[layer:layer + 1, :], activate)
        for half in range(2):
            wait_bytes(a_all.at[layer, 0:F_TEAM - F_OWN, 0:HALF], recv_sem.at[base + 3 + 2 * half])
            if half == 0:
                take(layer, 5)
                wait_bytes(wd_buf.at[layer, 0:F_TEAM - F_OWN], down_recv.at[layer])
            first = pairs[half] * (TEAMS // 2)
            part[layer, pl.ds(first, TEAMS // 2)] = dot_f32(
                a_all[layer, :, half_rows(half)], wd_buf[layer], ((0,), (0,))).reshape(TEAMS // 2, TEAM_ROWS, D_OWN)

            def scatter(i, carry, first=first):
                to = first + lax.rem(lax.rem(team, TEAMS // 2) + i, TEAMS // 2)
                remote(part.at[layer, to], land.at[layer, team], send_sem.at[base + 4], recv_sem.at[base + 4],
                       to * TEAM + slot).start()
                return carry

            lax.fori_loop(1 - half, TEAMS // 2, scatter, 0)
        pending.append((land.at[layer, 0:TEAMS - 1], send_sem.at[base + 4]))
        if layer + 1 < LAYERS:
            share_down(layer + 1)
        land[layer, team] = part[layer, team]
        wait_bytes(land.at[layer, 0:TEAMS - 1], recv_sem.at[base + 4])
        total = land[layer, 0]
        for i in range(1, TEAMS):
            total = total + land[layer, i]
        x_block = (x_block.astype(F32) + total).astype(BF16)

        if layer == 0:
            own_block = xb_team.at[:, own_cols]
            own_block[...] = x_block
            gather_team(own_block, own_block, 6)
            wait_bytes(xb_team.at[:, 0:D - D_OWN], recv_sem.at[6])
            x_team[...] = xb_team[...].astype(F32)
        else:
            gather_all(x_block, LAYERS, norm_final[...], lambda half: None)

    head_load.wait()
    copies = []
    for i, first in enumerate(range(0, VOCAB_OWN, HEAD_CHUNK)):
        size = min(HEAD_CHUNK, VOCAB_OWN - first)
        logits[first:first + size, :] = dot_f32(head_buf[first:first + size, :], g_buf[...], ((1,), (1,)))
        copies.append(pltpu.make_async_copy(logits.at[first:first + size], out.at[first:first + size], out_sem.at[i]))
        copies[-1].start()
    for copy in copies:
        copy.wait()
    for ref, sem in pending:
        wait_bytes(ref, sem)


def make_selectors(pack, spread):
    row = lax.broadcasted_iota(jnp.int32, pack.shape, 0)
    col = lax.broadcasted_iota(jnp.int32, pack.shape, 1)
    half = jnp.where(row >= HEADS, 1, 0)
    head = row - HEADS * half
    hit = col == half * 32 + (head & 1) * 16 + (head >> 1)
    pack[...] = jnp.where(hit, 1.0, 0.0).astype(BF16)
    shape = (TEAM_ROWS, TEAM_ROWS * O_ROWS)
    row = lax.broadcasted_iota(jnp.int32, shape, 0)
    col = lax.broadcasted_iota(jnp.int32, shape, 1)
    at = col - row * O_ROWS
    for i in range(O_ROWS):
        wanted = (i % 2) * HEADS + i // 2
        spread[i * TEAM_ROWS:(i + 1) * TEAM_ROWS, :] = jnp.where(at == wanted, 1.0, 0.0).astype(BF16)


def decode(hidden, lengths, kv_cache, norm_attn, w_q, w_o, norm_ffn, w_gate, w_up, w_down, norm_final, w_head):
    hbm = pl.BlockSpec(memory_space=pl.ANY)
    dma = pltpu.SemaphoreType.DMA
    return pl.pallas_call(
        decode_kernel,
        out_shape=jax.ShapeDtypeStruct((VOCAB_OWN, ALL_ROWS), F32),
        in_specs=[hbm] * 12,
        out_specs=hbm,
        scratch_shapes=[
            pltpu.VMEM((ROWS, D), BF16),
            pltpu.SMEM((ROWS,), jnp.int32),
            pltpu.VMEM((LAYERS, D), F32),
            pltpu.VMEM((LAYERS, D), F32),
            pltpu.VMEM((1, D), F32),
            pltpu.VMEM((VOCAB_OWN, D), BF16),
            pltpu.VMEM((VOCAB_OWN, ALL_ROWS), F32),
            pltpu.VMEM((O_ROWS, 64), BF16),
            pltpu.VMEM((O_ROWS * TEAM_ROWS, TEAM_ROWS * O_ROWS), BF16),
            pltpu.VMEM((TEAM, ROWS, D), BF16),
            pltpu.VMEM((TEAM_ROWS, D), F32),
            pltpu.VMEM((TEAM_ROWS, D), BF16),
            pltpu.VMEM((LAYERS, D, Q_OWN), BF16),
            pltpu.VMEM((LAYERS, ROWS, KV + 2 * SHIFT, SEQ), BF16),
            pltpu.VMEM((LAYERS, HEADS * LATENT, D_OWN), BF16),
            pltpu.VMEM((LAYERS, 2 * F_OWN, D), BF16),
            pltpu.VMEM((LAYERS, F_TEAM, D_OWN), BF16),
            pltpu.VMEM((LAYERS, TEAM, ROWS, Q_OWN), BF16),
            pltpu.VMEM((LAYERS, TEAM, ROWS, Q_OWN), BF16),
            pltpu.VMEM((ROWS, 16, PAIR), F32),
            pltpu.VMEM((LAYERS, ROWS, O_ROWS, O_COLS), BF16),
            pltpu.VMEM((LAYERS, TEAM, ROWS, O_ROWS, O_COLS), BF16),
            pltpu.VMEM((O_ROWS * TEAM_ROWS, O_COLS), BF16),
            pltpu.VMEM((LAYERS + 1, TEAMS, TEAM_ROWS, D), BF16),
            pltpu.VMEM((ALL_ROWS, D), BF16),
            pltpu.VMEM((LAYERS, F_TEAM, ALL_ROWS), BF16),
            pltpu.VMEM((LAYERS, TEAMS, TEAM_ROWS, D_OWN), F32),
            pltpu.VMEM((LAYERS, TEAMS, TEAM_ROWS, D_OWN), F32),
            dma((LAYERS, 6)),
            pltpu.SemaphoreType.REGULAR,
            dma((22,)),
            dma((22,)),
            dma((LAYERS + 1, 8)),
            dma((LAYERS,)),
            dma((LAYERS,)),
            dma((LAYERS, ROWS, 2)),
            dma,
            dma((-(-VOCAB_OWN // HEAD_CHUNK),)),
            dma((5,)),
        ],
        compiler_params=pltpu.CompilerParams(collective_id=0, has_side_effects=True, vmem_limit_bytes=60 * 1024 * 1024),
        name='decode',
    )(hidden, lengths, kv_cache, norm_attn, w_q, w_o, norm_ffn, w_gate, w_up, w_down, norm_final, w_head)


def solution(mesh):
    row_axes = ('rep', 'dp')
    specs_in = (P(row_axes, None), P(row_axes), P(None, row_axes, None, None), P(), P(), P(), P(),
                P(None, None, 'dp'), P(None, None, 'dp'), P(None, 'dp', None), P(), P(None, 'dp'))

    def device_step(hidden, lengths, kv_cache, norm_attn, w_q, w_o, norm_ffn, w_gate, w_up, w_down, norm_final, w_head):
        logits = decode(hidden, lengths, jnp.swapaxes(kv_cache, 2, 3), norm_attn, w_q, w_o, norm_ffn,
                        jnp.swapaxes(w_gate, 1, 2), jnp.swapaxes(w_up, 1, 2), w_down, norm_final.reshape(1, -1),
                        jnp.swapaxes(w_head, 0, 1))
        return jnp.swapaxes(logits, 0, 1)

    return jax.shard_map(device_step, mesh=mesh, in_specs=specs_in, out_specs=P('rep', 'dp'), check_vma=False)
```

```python
import jax
import jax.numpy as jnp
from jax import lax
from jax.experimental import pallas as pl
from jax.experimental.pallas import tpu as pltpu
from jax.sharding import PartitionSpec as P

MESH = pl.DeviceIdType.MESH
QK_SCALE = 192 ** -0.5
NORM_EPS = 1e-6

LAYERS = 2
ROWS = 2
TEAM = 8
TEAMS = 16
TEAM_ROWS = ROWS * TEAM
ALL_ROWS = TEAM_ROWS * TEAMS
HALF = ALL_ROWS // 2
D = 2048
D_OWN = D // TEAM
HEADS = 20
LATENT = 512
KV = 576
SEQ = 512
Q_COLS = HEADS * KV
Q_OWN = 1536
Q_LAST = Q_COLS - Q_OWN
PAIR = 2 * KV
PAIRS = HEADS // 2
SHIFT = 64
WIDE = KV + SHIFT
O_ROWS = 2 * HEADS
O_COLS = LATENT // 2
F_OWN = 80
F_TEAM = F_OWN * TEAM
VOCAB_OWN = 1210
HEAD_CHUNK = 304
F32 = jnp.float32
BF16 = jnp.bfloat16


def norm_rows(x, gain):
    inv_rms = lax.rsqrt(jnp.mean(x * x, axis=-1, keepdims=True) + NORM_EPS)
    return (x * inv_rms * gain).astype(BF16)


def dot_f32(a, b, contract=((1,), (0,))):
    return lax.dot_general(a, b, (contract, ((), ())), preferred_element_type=F32)


def wait_bytes(ref, sem):
    pltpu.make_async_copy(ref, ref, sem).wait()


def q_segments():
    pieces = []
    for pair in range(PAIRS):
        at, end = pair * PAIR, (pair + 1) * PAIR
        while at < end:
            sender = at // Q_OWN
            first = min(sender * Q_OWN, Q_LAST)
            stop = min(end, (sender + 1) * Q_OWN, Q_COLS)
            pieces.append((pair, at - pair * PAIR, sender, at - first, stop - at))
            at = stop
    return pieces


def decode_kernel(hidden, lengths, kv_cache, norm_attn, w_q, w_o, norm_ffn, w_gate, w_up, w_down, norm_final, w_head,
                  out, head_buf, logits, pack, spread, hid_land, x_team, xb_team, wq_buf, kv_buf, wo_buf, wgu_buf, wd_buf,
                  q_send, q_land, q_pairs, o_send, o_land, o_heads, x_all, g_buf, a_all, part, land,
                  load_sem, entry_sem, send_sem, recv_sem, plane_sem, down_send, down_recv, near_sem, head_sem, out_sem):
    me = lax.axis_index('dp')
    team, slot = me // TEAM, lax.rem(me, TEAM)
    plane, core = team // 4, lax.rem(me, 2)
    sibling = me + 1 - 2 * core
    own_cols = pl.ds(pl.multiple_of(slot * D_OWN, D_OWN), D_OWN)
    q_start = pl.multiple_of(jnp.minimum(slot * Q_OWN, Q_LAST), 128)

    pending = []

    def take(layer, i):
        loads[layer][i].wait()

    def mate(i):
        return team * TEAM + lax.rem(slot + i, TEAM)

    def remote(src, dst, ssem, rsem, device):
        return pltpu.make_async_remote_copy(src, dst, ssem, rsem, device_id={'dp': device}, device_id_type=MESH)

    barrier = pltpu.get_barrier_semaphore()
    for i in range(1, TEAM):
        pl.semaphore_signal(barrier, inc=1, device_id={'dp': mate(i)}, device_id_type=MESH)

    def greet(i, carry):
        pl.semaphore_signal(barrier, inc=1, device_id={'dp': lax.rem(me + i * TEAM, TEAM * TEAMS)}, device_id_type=MESH)
        return carry

    lax.fori_loop(1, TEAMS, greet, 0)

    loads = []
    for layer in range(LAYERS):
        batch = [
            (w_q.at[layer, :, pl.ds(q_start, Q_OWN)], wq_buf.at[layer]),
            (kv_cache.at[layer], kv_buf.at[layer, :, pl.ds(SHIFT, KV)]),
            (w_o.at[layer, :, own_cols], wo_buf.at[layer]),
            (w_gate.at[layer], wgu_buf.at[layer, pl.ds(0, F_OWN)]),
            (w_up.at[layer], wgu_buf.at[layer, pl.ds(F_OWN, F_OWN)]),
            (w_down.at[layer, :, own_cols], wd_buf.at[layer, pl.ds(pl.multiple_of(slot * F_OWN, 16), F_OWN)]),
        ]
        loads.append([pltpu.make_async_copy(src, dst, load_sem.at[layer, i]) for i, (src, dst) in enumerate(batch)])
    for batch in loads:
        for copy in batch:
            copy.start()
    head_load = pltpu.make_async_copy(w_head, head_buf, head_sem)
    head_load.start()

    for layer in range(LAYERS):
        for r in range(ROWS):
            kv_buf[layer, r, 0:SHIFT, :] = jnp.zeros((SHIFT, SEQ), BF16)
            kv_buf[layer, r, SHIFT + KV:, :] = jnp.zeros((SHIFT, SEQ), BF16)
    q_pairs[...] = jnp.zeros_like(q_pairs)
    make_selectors(pack, spread)
    hid_land[slot] = hidden[...]

    pl.semaphore_wait(barrier, TEAM - 1 + TEAMS - 1)
    for i in range(1, TEAM):
        pl.semaphore_signal(entry_sem, inc=1, device_id={'dp': mate(i)}, device_id_type=MESH)

    def gather_team(src, dst, sem):
        for i in range(1, TEAM):
            remote(src, dst, send_sem.at[sem], recv_sem.at[sem], mate(i)).start()
            pending.append((src, send_sem.at[sem]))

    def share_down(layer):
        for i in range(1, TEAM):
            to = lax.rem(slot + i, TEAM)
            remote(w_down.at[layer, :, pl.ds(pl.multiple_of(to * D_OWN, D_OWN), D_OWN)],
                   wd_buf.at[layer, pl.ds(pl.multiple_of(slot * F_OWN, 16), F_OWN)],
                   down_send.at[layer], down_recv.at[layer], mate(i)).start()
        pending.append((wd_buf.at[layer, 0:F_TEAM - F_OWN], down_send.at[layer]))

    def gather_all(block, step, gain, use_half):
        dst = x_all.at[step]
        mine = dst.at[team, :, own_cols]
        mine[...] = block
        direct, passed = send_sem.at[16 + 2 * step], send_sem.at[17 + 2 * step]
        planes = (plane, plane + 1 - 2 * lax.rem(plane, 2), 3 - plane, lax.rem(plane + 2, 4))
        for k in (1, 0, 3, 2):

            def send(i, carry, k=k):
                spot = lax.rem(lax.rem(me, 32) // 2 + 24 - i, 16)
                remote(mine, mine, direct, plane_sem.at[step, k], planes[k] * 32 + spot * 2 + core).start()
                return carry

            def send_near(i, carry, k=k):
                spot = lax.rem(lax.rem(me, 32) // 2 + i, 16)
                remote(mine, mine, direct, plane_sem.at[step, k], planes[k] * 32 + spot * 2 + core).start()
                return carry

            if k:
                lax.fori_loop(0, 16, send, 0)
            else:
                lax.fori_loop(1, 16, send_near, 0)
        pending.append((dst.at[0:7], direct))
        pending.append((dst.at[0, :, 0:7 * D_OWN], direct))
        pending.append((dst.at[0:8], passed))

        def finish(k):
            wait_bytes(dst.at[0:4, :, 0:4 * D_OWN], plane_sem.at[step, 4 + k])

            def chunk(i, carry):
                row = planes[k] * 4 + i
                g_buf[pl.ds(pl.multiple_of(row * TEAM_ROWS, TEAM_ROWS), TEAM_ROWS), :] = norm_rows(
                    dst[row].astype(F32), gain)
                return carry

            lax.fori_loop(0, 4, chunk, 0)

        for half in range(2):
            for k in (2 * half, 2 * half + 1):
                if k == 0:
                    wait_bytes(dst.at[0:3, :, 0:5 * D_OWN], plane_sem.at[step, k])
                else:
                    wait_bytes(dst.at[0:4, :, 0:4 * D_OWN], plane_sem.at[step, k])
                for x in range(4):
                    cols = pl.ds(pl.multiple_of((2 * x + core) * D_OWN, D_OWN), D_OWN)
                    piece = dst.at[pl.ds(planes[k] * 4, 4), :, cols]
                    remote(piece, piece, passed, plane_sem.at[step, 4 + k], sibling).start()
            finish(2 * half)
            finish(2 * half + 1)
            use_half(half)

    gather_team(hidden, hid_land.at[slot], 0)
    share_down(0)
    wait_bytes(hid_land.at[0:TEAM - 1], recv_sem.at[0])
    for i in range(TEAM):
        x_team[ROWS * i:ROWS * (i + 1), :] = hid_land[i].astype(F32)

    for layer in range(LAYERS):
        base = 8 * layer
        h = norm_rows(x_team[...], norm_attn[layer:layer + 1, :])
        x_block = x_team[:, own_cols]
        take(layer, 0)
        for c in range(Q_OWN // 256):
            cols = slice(c * 256, (c + 1) * 256)
            q = dot_f32(h, wq_buf[layer, :, cols])
            for i in range(TEAM):
                q_send[layer, i, :, cols] = q[ROWS * i:ROWS * (i + 1), :].astype(BF16)
        for i in range(1, TEAM):
            to = lax.rem(slot + i, TEAM)
            remote(q_send.at[layer, to], q_land.at[layer, slot], send_sem.at[base + 1], recv_sem.at[base + 1],
                   mate(i)).start()
        pending.append((q_land.at[layer, 0:TEAM - 1], send_sem.at[base + 1]))
        q_land[layer, slot] = q_send[layer, slot]
        wait_bytes(q_land.at[layer, 0:TEAM - 1], recv_sem.at[base + 1])
        for pair, at, sender, col, width in q_segments():
            piece = q_land[layer, sender, :, col:col + width].astype(F32)
            for r in range(ROWS):
                q_pairs[r, pair:pair + 1, at:at + width] = piece[r:r + 1]

        take(layer, 1)
        lane = lax.broadcasted_iota(jnp.int32, (16, WIDE), 1)
        key_pos = lax.broadcasted_iota(jnp.int32, (32, SEQ), 1)
        for r in range(ROWS):
            q_even = jnp.where(lane < KV, q_pairs[r, :, 0:WIDE], 0.0).astype(BF16)
            q_odd = jnp.where(lane >= SHIFT, q_pairs[r, :, PAIR - WIDE:PAIR], 0.0).astype(BF16)
            scores = jnp.concatenate([dot_f32(q_even, kv_buf[layer, r, SHIFT:SHIFT + WIDE, :]),
                                      dot_f32(q_odd, kv_buf[layer, r, 0:WIDE, :])], axis=0) * QK_SCALE
            scores = jnp.where(key_pos < lengths[r], scores, -1e30)
            weights = jnp.exp(scores - jnp.max(scores, axis=-1, keepdims=True))
            probs = (weights / jnp.sum(weights, axis=-1, keepdims=True)).astype(BF16)
            context = dot_f32(probs, kv_buf[layer, r, SHIFT:SHIFT + LATENT, :], ((1,), (1,))).astype(BF16)
            halves = jnp.concatenate([context[:, :O_COLS], context[:, O_COLS:]], axis=0)
            o_send[layer, r] = dot_f32(pack[...], halves).astype(BF16)
            block, dst = o_send.at[layer, r], o_land.at[layer, slot, r]
            osem, orecv = send_sem.at[base + 2], recv_sem.at[base + 2]
            remote(block, dst, osem, near_sem.at[layer, r, 2], mate(4)).start()
            remote(block, dst, osem, near_sem.at[layer, r, 0], mate(2)).start()
            remote(block, dst, osem, near_sem.at[layer, r, 1], mate(TEAM - 2)).start()
            remote(block, dst, osem, orecv, sibling).start()
            o_land[layer, slot, r] = o_send[layer, r]
            pending.extend([(block, osem)] * (TEAM - 1))
        for r in range(ROWS):
            for side, i in enumerate((TEAM - 2, 2, 4)):
                piece = o_land.at[layer, lax.rem(slot + i, TEAM), r]
                wait_bytes(piece, near_sem.at[layer, r, side])
                remote(piece, piece, send_sem.at[base + 2], recv_sem.at[base + 2], sibling).start()
        wait_bytes(o_land.at[layer, 0:TEAM // 2], recv_sem.at[base + 2])

        o_heads[...] = dot_f32(spread[...], o_land[layer].reshape(TEAM_ROWS * O_ROWS, O_COLS)).astype(BF16)
        take(layer, 2)

        heads = jnp.concatenate([o_heads[i * TEAM_ROWS:(i + 1) * TEAM_ROWS, :] for i in range(O_ROWS)], axis=1)
        delta = dot_f32(heads, wo_buf[layer])
        x_block = (x_block + delta).astype(BF16)
        if layer == 0:
            pl.semaphore_wait(entry_sem, TEAM - 1)
        own_pair = plane // 2
        pairs = (own_pair, 1 - own_pair)

        def half_rows(half):
            return pl.ds(pl.multiple_of(pairs[half] * HALF, HALF), HALF)

        def activate(half, layer=layer, base=base):
            if half == 0:
                take(layer, 3)
                take(layer, 4)
            gate_up = dot_f32(wgu_buf[layer], g_buf[half_rows(half), :], ((1,), (1,)))
            act = (jax.nn.silu(gate_up[0:F_OWN]) * gate_up[F_OWN:]).astype(BF16)
            own_hidden = a_all.at[layer, pl.ds(pl.multiple_of(slot * F_OWN, 16), F_OWN), half_rows(half)]
            own_hidden[...] = act
            gather_team(own_hidden, own_hidden, base + 3 + 2 * half)

        gather_all(x_block, layer, norm_ffn[layer:layer + 1, :], activate)
        for half in range(2):
            wait_bytes(a_all.at[layer, 0:F_TEAM - F_OWN, 0:HALF], recv_sem.at[base + 3 + 2 * half])
            if half == 0:
                take(layer, 5)
                wait_bytes(wd_buf.at[layer, 0:F_TEAM - F_OWN], down_recv.at[layer])
            first = pairs[half] * (TEAMS // 2)
            part[layer, pl.ds(first, TEAMS // 2)] = dot_f32(
                a_all[layer, :, half_rows(half)], wd_buf[layer], ((0,), (0,))).reshape(TEAMS // 2, TEAM_ROWS, D_OWN)

            def scatter(i, carry, first=first):
                to = first + lax.rem(lax.rem(team, TEAMS // 2) + i, TEAMS // 2)
                remote(part.at[layer, to], land.at[layer, team], send_sem.at[base + 4], recv_sem.at[base + 4],
                       to * TEAM + slot).start()
                return carry

            lax.fori_loop(1 - half, TEAMS // 2, scatter, 0)
        pending.append((land.at[layer, 0:TEAMS - 1], send_sem.at[base + 4]))
        if layer + 1 < LAYERS:
            share_down(layer + 1)
        land[layer, team] = part[layer, team]
        wait_bytes(land.at[layer, 0:TEAMS - 1], recv_sem.at[base + 4])
        total = land[layer, 0]
        for i in range(1, TEAMS):
            total = total + land[layer, i]
        x_block = (x_block.astype(F32) + total).astype(BF16)

        if layer == 0:
            own_block = xb_team.at[:, own_cols]
            own_block[...] = x_block
            gather_team(own_block, own_block, 6)
            wait_bytes(xb_team.at[:, 0:D - D_OWN], recv_sem.at[6])
            x_team[...] = xb_team[...].astype(F32)
        else:
            gather_all(x_block, LAYERS, norm_final[...], lambda half: None)

    head_load.wait()
    copies = []
    for i, first in enumerate(range(0, VOCAB_OWN, HEAD_CHUNK)):
        size = min(HEAD_CHUNK, VOCAB_OWN - first)
        logits[first:first + size, :] = dot_f32(head_buf[first:first + size, :], g_buf[...], ((1,), (1,)))
        copies.append(pltpu.make_async_copy(logits.at[first:first + size], out.at[first:first + size], out_sem.at[i]))
        copies[-1].start()
    for copy in copies:
        copy.wait()
    for ref, sem in pending:
        wait_bytes(ref, sem)


def make_selectors(pack, spread):
    row = lax.broadcasted_iota(jnp.int32, pack.shape, 0)
    col = lax.broadcasted_iota(jnp.int32, pack.shape, 1)
    half = jnp.where(row >= HEADS, 1, 0)
    head = row - HEADS * half
    hit = col == half * 32 + (head & 1) * 16 + (head >> 1)
    pack[...] = jnp.where(hit, 1.0, 0.0).astype(BF16)
    shape = (TEAM_ROWS, TEAM_ROWS * O_ROWS)
    row = lax.broadcasted_iota(jnp.int32, shape, 0)
    col = lax.broadcasted_iota(jnp.int32, shape, 1)
    at = col - row * O_ROWS
    for i in range(O_ROWS):
        wanted = (i % 2) * HEADS + i // 2
        spread[i * TEAM_ROWS:(i + 1) * TEAM_ROWS, :] = jnp.where(at == wanted, 1.0, 0.0).astype(BF16)


def decode(hidden, lengths, kv_cache, norm_attn, w_q, w_o, norm_ffn, w_gate, w_up, w_down, norm_final, w_head):
    vmem = pl.BlockSpec(memory_space=pltpu.VMEM)
    smem = pl.BlockSpec(memory_space=pltpu.SMEM)
    hbm = pl.BlockSpec(memory_space=pl.ANY)
    dma = pltpu.SemaphoreType.DMA
    return pl.pallas_call(
        decode_kernel,
        out_shape=jax.ShapeDtypeStruct((VOCAB_OWN, ALL_ROWS), F32),
        in_specs=[vmem, smem, hbm, vmem, hbm, hbm, vmem, hbm, hbm, hbm, vmem, hbm],
        out_specs=hbm,
        scratch_shapes=[
            pltpu.VMEM((VOCAB_OWN, D), BF16),
            pltpu.VMEM((VOCAB_OWN, ALL_ROWS), F32),
            pltpu.VMEM((O_ROWS, 64), BF16),
            pltpu.VMEM((O_ROWS * TEAM_ROWS, TEAM_ROWS * O_ROWS), BF16),
            pltpu.VMEM((TEAM, ROWS, D), BF16),
            pltpu.VMEM((TEAM_ROWS, D), F32),
            pltpu.VMEM((TEAM_ROWS, D), BF16),
            pltpu.VMEM((LAYERS, D, Q_OWN), BF16),
            pltpu.VMEM((LAYERS, ROWS, KV + 2 * SHIFT, SEQ), BF16),
            pltpu.VMEM((LAYERS, HEADS * LATENT, D_OWN), BF16),
            pltpu.VMEM((LAYERS, 2 * F_OWN, D), BF16),
            pltpu.VMEM((LAYERS, F_TEAM, D_OWN), BF16),
            pltpu.VMEM((LAYERS, TEAM, ROWS, Q_OWN), BF16),
            pltpu.VMEM((LAYERS, TEAM, ROWS, Q_OWN), BF16),
            pltpu.VMEM((ROWS, 16, PAIR), F32),
            pltpu.VMEM((LAYERS, ROWS, O_ROWS, O_COLS), BF16),
            pltpu.VMEM((LAYERS, TEAM, ROWS, O_ROWS, O_COLS), BF16),
            pltpu.VMEM((O_ROWS * TEAM_ROWS, O_COLS), BF16),
            pltpu.VMEM((LAYERS + 1, TEAMS, TEAM_ROWS, D), BF16),
            pltpu.VMEM((ALL_ROWS, D), BF16),
            pltpu.VMEM((LAYERS, F_TEAM, ALL_ROWS), BF16),
            pltpu.VMEM((LAYERS, TEAMS, TEAM_ROWS, D_OWN), F32),
            pltpu.VMEM((LAYERS, TEAMS, TEAM_ROWS, D_OWN), F32),
            dma((LAYERS, 6)),
            pltpu.SemaphoreType.REGULAR,
            dma((22,)),
            dma((22,)),
            dma((LAYERS + 1, 8)),
            dma((LAYERS,)),
            dma((LAYERS,)),
            dma((LAYERS, ROWS, 3)),
            dma,
            dma((-(-VOCAB_OWN // HEAD_CHUNK),)),
        ],
        compiler_params=pltpu.CompilerParams(collective_id=0, has_side_effects=True, vmem_limit_bytes=60 * 1024 * 1024),
        name='decode',
    )(hidden, lengths, kv_cache, norm_attn, w_q, w_o, norm_ffn, w_gate, w_up, w_down, norm_final, w_head)


def solution(mesh):
    row_axes = ('rep', 'dp')
    specs_in = (P(row_axes, None), P(row_axes), P(None, row_axes, None, None), P(), P(), P(), P(),
                P(None, None, 'dp'), P(None, None, 'dp'), P(None, 'dp', None), P(), P(None, 'dp'))

    def device_step(hidden, lengths, kv_cache, norm_attn, w_q, w_o, norm_ffn, w_gate, w_up, w_down, norm_final, w_head):
        logits = decode(hidden, lengths, jnp.swapaxes(kv_cache, 2, 3), norm_attn, w_q, w_o, norm_ffn,
                        jnp.swapaxes(w_gate, 1, 2), jnp.swapaxes(w_up, 1, 2), w_down, norm_final.reshape(1, -1),
                        jnp.swapaxes(w_head, 0, 1))
        return jnp.swapaxes(logits, 0, 1)

    return jax.shard_map(device_step, mesh=mesh, in_specs=specs_in, out_specs=P('rep', 'dp'), check_vma=False)
```

```python
import jax
import jax.numpy as jnp
from jax import lax
from jax.experimental import pallas as pl
from jax.experimental.pallas import tpu as pltpu
from jax.sharding import PartitionSpec as P

MESH = pl.DeviceIdType.MESH
QK_SCALE = 192 ** -0.5
NORM_EPS = 1e-6

LAYERS = 2
ROWS = 2
TEAM = 8
TEAMS = 16
TEAM_ROWS = ROWS * TEAM
ALL_ROWS = TEAM_ROWS * TEAMS
HALF = ALL_ROWS // 2
D = 2048
D_OWN = D // TEAM
HEADS = 20
LATENT = 512
KV = 576
SEQ = 512
Q_COLS = HEADS * KV
Q_OWN = 1536
Q_LAST = Q_COLS - Q_OWN
PAIR = 2 * KV
PAIRS = HEADS // 2
SHIFT = 64
WIDE = KV + SHIFT
O_ROWS = 2 * HEADS
O_COLS = LATENT // 2
F_OWN = 80
F_TEAM = F_OWN * TEAM
VOCAB_OWN = 1210
HEAD_CHUNK = 304
F32 = jnp.float32
BF16 = jnp.bfloat16


def norm_rows(x, gain):
    inv_rms = lax.rsqrt(jnp.mean(x * x, axis=-1, keepdims=True) + NORM_EPS)
    return (x * inv_rms * gain).astype(BF16)


def dot_f32(a, b, contract=((1,), (0,))):
    return lax.dot_general(a, b, (contract, ((), ())), preferred_element_type=F32)


def wait_bytes(ref, sem):
    pltpu.make_async_copy(ref, ref, sem).wait()


def q_segments():
    pieces = []
    for pair in range(PAIRS):
        at, end = pair * PAIR, (pair + 1) * PAIR
        while at < end:
            sender = at // Q_OWN
            first = min(sender * Q_OWN, Q_LAST)
            stop = min(end, (sender + 1) * Q_OWN, Q_COLS)
            pieces.append((pair, at - pair * PAIR, sender, at - first, stop - at))
            at = stop
    return pieces


def decode_kernel(hidden_in, lengths_in, kv_cache, norm_attn_in, w_q, w_o, norm_ffn_in, w_gate, w_up, w_down, norm_final_in, w_head,
                  out, hidden, lengths, norm_attn, norm_ffn, norm_final, head_buf, logits, pack, spread, hid_land, x_team, xb_team, wq_buf, kv_buf, wo_buf, wgu_buf, wd_buf,
                  q_send, q_land, q_pairs, o_send, o_land, o_heads, x_all, g_buf, a_all, part, land,
                  load_sem, entry_sem, send_sem, recv_sem, plane_sem, down_send, down_recv, near_sem, head_sem, out_sem, small_sem):
    me = lax.axis_index('dp')
    team, slot = me // TEAM, lax.rem(me, TEAM)
    plane, core = team // 4, lax.rem(me, 2)
    sibling = me + 1 - 2 * core
    own_cols = pl.ds(pl.multiple_of(slot * D_OWN, D_OWN), D_OWN)
    q_start = pl.multiple_of(jnp.minimum(slot * Q_OWN, Q_LAST), 128)

    pending = []

    def take(layer, i):
        loads[layer][i].wait()

    def mate(i):
        return team * TEAM + lax.rem(slot + i, TEAM)

    def remote(src, dst, ssem, rsem, device):
        return pltpu.make_async_remote_copy(src, dst, ssem, rsem, device_id={'dp': device}, device_id_type=MESH)

    barrier = pltpu.get_barrier_semaphore()
    for i in range(1, TEAM):
        pl.semaphore_signal(barrier, inc=1, device_id={'dp': mate(i)}, device_id_type=MESH)

    def greet(i, carry):
        pl.semaphore_signal(barrier, inc=1, device_id={'dp': lax.rem(me + i * TEAM, TEAM * TEAMS)}, device_id_type=MESH)
        return carry

    lax.fori_loop(1, TEAMS, greet, 0)

    smalls = [pltpu.make_async_copy(src, dst, small_sem.at[i]) for i, (src, dst) in enumerate((
        (hidden_in, hidden), (norm_attn_in, norm_attn), (lengths_in, lengths), (norm_ffn_in, norm_ffn),
        (norm_final_in, norm_final)))]
    for copy in smalls:
        copy.start()
    q_pairs[...] = jnp.zeros_like(q_pairs)
    make_selectors(pack, spread)
    for copy in smalls:
        copy.wait()

    loads = []
    for layer in range(LAYERS):
        batch = [
            (w_q.at[layer, :, pl.ds(q_start, Q_OWN)], wq_buf.at[layer]),
            (kv_cache.at[layer], kv_buf.at[layer, :, pl.ds(SHIFT, KV)]),
            (w_o.at[layer, :, own_cols], wo_buf.at[layer]),
            (w_gate.at[layer], wgu_buf.at[layer, pl.ds(0, F_OWN)]),
            (w_up.at[layer], wgu_buf.at[layer, pl.ds(F_OWN, F_OWN)]),
            (w_down.at[layer, :, own_cols], wd_buf.at[layer, pl.ds(pl.multiple_of(slot * F_OWN, 16), F_OWN)]),
        ]
        loads.append([pltpu.make_async_copy(src, dst, load_sem.at[layer, i]) for i, (src, dst) in enumerate(batch)])
    for batch in loads:
        for copy in batch:
            copy.start()
    head_load = pltpu.make_async_copy(w_head, head_buf, head_sem)
    head_load.start()

    for layer in range(LAYERS):
        for r in range(ROWS):
            kv_buf[layer, r, 0:SHIFT, :] = jnp.zeros((SHIFT, SEQ), BF16)
            kv_buf[layer, r, SHIFT + KV:, :] = jnp.zeros((SHIFT, SEQ), BF16)
    hid_land[slot] = hidden[...]

    pl.semaphore_wait(barrier, TEAM - 1 + TEAMS - 1)
    for i in range(1, TEAM):
        pl.semaphore_signal(entry_sem, inc=1, device_id={'dp': mate(i)}, device_id_type=MESH)

    def gather_team(src, dst, sem):
        for i in range(1, TEAM):
            remote(src, dst, send_sem.at[sem], recv_sem.at[sem], mate(i)).start()
            pending.append((src, send_sem.at[sem]))

    def share_down(layer):
        for i in range(1, TEAM):
            to = lax.rem(slot + i, TEAM)
            remote(w_down.at[layer, :, pl.ds(pl.multiple_of(to * D_OWN, D_OWN), D_OWN)],
                   wd_buf.at[layer, pl.ds(pl.multiple_of(slot * F_OWN, 16), F_OWN)],
                   down_send.at[layer], down_recv.at[layer], mate(i)).start()
        pending.append((wd_buf.at[layer, 0:F_TEAM - F_OWN], down_send.at[layer]))

    def gather_all(block, step, gain, use_half):
        dst = x_all.at[step]
        mine = dst.at[team, :, own_cols]
        mine[...] = block
        direct, passed = send_sem.at[16 + 2 * step], send_sem.at[17 + 2 * step]
        planes = (plane, plane + 1 - 2 * lax.rem(plane, 2), 3 - plane, lax.rem(plane + 2, 4))
        for k in (1, 0, 3, 2):

            def send(i, carry, k=k):
                spot = lax.rem(lax.rem(me, 32) // 2 + 24 - i, 16)
                remote(mine, mine, direct, plane_sem.at[step, k], planes[k] * 32 + spot * 2 + core).start()
                return carry

            def send_near(i, carry, k=k):
                spot = lax.rem(lax.rem(me, 32) // 2 + i, 16)
                remote(mine, mine, direct, plane_sem.at[step, k], planes[k] * 32 + spot * 2 + core).start()
                return carry

            if k:
                lax.fori_loop(0, 16, send, 0)
            else:
                lax.fori_loop(1, 16, send_near, 0)
        pending.append((dst.at[0:7], direct))
        pending.append((dst.at[0, :, 0:7 * D_OWN], direct))
        pending.append((dst.at[0:8], passed))

        def finish(k):
            wait_bytes(dst.at[0:4, :, 0:4 * D_OWN], plane_sem.at[step, 4 + k])

            def chunk(i, carry):
                row = planes[k] * 4 + i
                g_buf[pl.ds(pl.multiple_of(row * TEAM_ROWS, TEAM_ROWS), TEAM_ROWS), :] = norm_rows(
                    dst[row].astype(F32), gain)
                return carry

            lax.fori_loop(0, 4, chunk, 0)

        for half in range(2):
            for k in (2 * half, 2 * half + 1):
                if k == 0:
                    wait_bytes(dst.at[0:3, :, 0:5 * D_OWN], plane_sem.at[step, k])
                else:
                    wait_bytes(dst.at[0:4, :, 0:4 * D_OWN], plane_sem.at[step, k])
                for x in range(4):
                    cols = pl.ds(pl.multiple_of((2 * x + core) * D_OWN, D_OWN), D_OWN)
                    piece = dst.at[pl.ds(planes[k] * 4, 4), :, cols]
                    remote(piece, piece, passed, plane_sem.at[step, 4 + k], sibling).start()
            finish(2 * half)
            finish(2 * half + 1)
            use_half(half)

    gather_team(hidden, hid_land.at[slot], 0)
    share_down(0)
    wait_bytes(hid_land.at[0:TEAM - 1], recv_sem.at[0])
    for i in range(TEAM):
        x_team[ROWS * i:ROWS * (i + 1), :] = hid_land[i].astype(F32)

    for layer in range(LAYERS):
        base = 8 * layer
        h = norm_rows(x_team[...], norm_attn[layer:layer + 1, :])
        x_block = x_team[:, own_cols]
        take(layer, 0)
        for c in range(Q_OWN // 256):
            cols = slice(c * 256, (c + 1) * 256)
            q = dot_f32(h, wq_buf[layer, :, cols])
            for i in range(TEAM):
                q_send[layer, i, :, cols] = q[ROWS * i:ROWS * (i + 1), :].astype(BF16)
        for i in range(1, TEAM):
            to = lax.rem(slot + i, TEAM)
            remote(q_send.at[layer, to], q_land.at[layer, slot], send_sem.at[base + 1], recv_sem.at[base + 1],
                   mate(i)).start()
        pending.append((q_land.at[layer, 0:TEAM - 1], send_sem.at[base + 1]))
        q_land[layer, slot] = q_send[layer, slot]
        wait_bytes(q_land.at[layer, 0:TEAM - 1], recv_sem.at[base + 1])
        for pair, at, sender, col, width in q_segments():
            piece = q_land[layer, sender, :, col:col + width].astype(F32)
            for r in range(ROWS):
                q_pairs[r, pair:pair + 1, at:at + width] = piece[r:r + 1]

        take(layer, 1)
        lane = lax.broadcasted_iota(jnp.int32, (16, WIDE), 1)
        key_pos = lax.broadcasted_iota(jnp.int32, (32, SEQ), 1)
        for r in range(ROWS):
            q_even = jnp.where(lane < KV, q_pairs[r, :, 0:WIDE], 0.0).astype(BF16)
            q_odd = jnp.where(lane >= SHIFT, q_pairs[r, :, PAIR - WIDE:PAIR], 0.0).astype(BF16)
            scores = jnp.concatenate([dot_f32(q_even, kv_buf[layer, r, SHIFT:SHIFT + WIDE, :]),
                                      dot_f32(q_odd, kv_buf[layer, r, 0:WIDE, :])], axis=0) * QK_SCALE
            scores = jnp.where(key_pos < lengths[r], scores, -1e30)
            weights = jnp.exp(scores - jnp.max(scores, axis=-1, keepdims=True))
            probs = (weights / jnp.sum(weights, axis=-1, keepdims=True)).astype(BF16)
            context = dot_f32(probs, kv_buf[layer, r, SHIFT:SHIFT + LATENT, :], ((1,), (1,))).astype(BF16)
            halves = jnp.concatenate([context[:, :O_COLS], context[:, O_COLS:]], axis=0)
            o_send[layer, r] = dot_f32(pack[...], halves).astype(BF16)
            block, dst = o_send.at[layer, r], o_land.at[layer, slot, r]
            osem, orecv = send_sem.at[base + 2], recv_sem.at[base + 2]
            remote(block, dst, osem, near_sem.at[layer, r, 2], mate(4)).start()
            remote(block, dst, osem, near_sem.at[layer, r, 0], mate(2)).start()
            remote(block, dst, osem, near_sem.at[layer, r, 1], mate(TEAM - 2)).start()
            remote(block, dst, osem, orecv, sibling).start()
            o_land[layer, slot, r] = o_send[layer, r]
            pending.extend([(block, osem)] * (TEAM - 1))
        for r in range(ROWS):
            for side, i in enumerate((TEAM - 2, 2, 4)):
                piece = o_land.at[layer, lax.rem(slot + i, TEAM), r]
                wait_bytes(piece, near_sem.at[layer, r, side])
                remote(piece, piece, send_sem.at[base + 2], recv_sem.at[base + 2], sibling).start()
        wait_bytes(o_land.at[layer, 0:TEAM // 2], recv_sem.at[base + 2])

        o_heads[...] = dot_f32(spread[...], o_land[layer].reshape(TEAM_ROWS * O_ROWS, O_COLS)).astype(BF16)
        take(layer, 2)

        heads = jnp.concatenate([o_heads[i * TEAM_ROWS:(i + 1) * TEAM_ROWS, :] for i in range(O_ROWS)], axis=1)
        delta = dot_f32(heads, wo_buf[layer])
        x_block = (x_block + delta).astype(BF16)
        if layer == 0:
            pl.semaphore_wait(entry_sem, TEAM - 1)
        own_pair = plane // 2
        pairs = (own_pair, 1 - own_pair)

        def half_rows(half):
            return pl.ds(pl.multiple_of(pairs[half] * HALF, HALF), HALF)

        def activate(half, layer=layer, base=base):
            if half == 0:
                take(layer, 3)
                take(layer, 4)
            gate_up = dot_f32(wgu_buf[layer], g_buf[half_rows(half), :], ((1,), (1,)))
            act = (jax.nn.silu(gate_up[0:F_OWN]) * gate_up[F_OWN:]).astype(BF16)
            own_hidden = a_all.at[layer, pl.ds(pl.multiple_of(slot * F_OWN, 16), F_OWN), half_rows(half)]
            own_hidden[...] = act
            gather_team(own_hidden, own_hidden, base + 3 + 2 * half)

        gather_all(x_block, layer, norm_ffn[layer:layer + 1, :], activate)
        for half in range(2):
            wait_bytes(a_all.at[layer, 0:F_TEAM - F_OWN, 0:HALF], recv_sem.at[base + 3 + 2 * half])
            if half == 0:
                take(layer, 5)
                wait_bytes(wd_buf.at[layer, 0:F_TEAM - F_OWN], down_recv.at[layer])
            first = pairs[half] * (TEAMS // 2)
            part[layer, pl.ds(first, TEAMS // 2)] = dot_f32(
                a_all[layer, :, half_rows(half)], wd_buf[layer], ((0,), (0,))).reshape(TEAMS // 2, TEAM_ROWS, D_OWN)

            def scatter(i, carry, first=first):
                to = first + lax.rem(lax.rem(team, TEAMS // 2) + TEAMS // 2 - i, TEAMS // 2)
                remote(part.at[layer, to], land.at[layer, team], send_sem.at[base + 4], recv_sem.at[base + 4],
                       to * TEAM + slot).start()
                return carry

            lax.fori_loop(1 - half, TEAMS // 2, scatter, 0)
        pending.append((land.at[layer, 0:TEAMS - 1], send_sem.at[base + 4]))
        if layer + 1 < LAYERS:
            share_down(layer + 1)
        land[layer, team] = part[layer, team]
        wait_bytes(land.at[layer, 0:TEAMS - 1], recv_sem.at[base + 4])
        total = land[layer, 0]
        for i in range(1, TEAMS):
            total = total + land[layer, i]
        x_block = (x_block.astype(F32) + total).astype(BF16)

        if layer == 0:
            own_block = xb_team.at[:, own_cols]
            own_block[...] = x_block
            gather_team(own_block, own_block, 6)
            wait_bytes(xb_team.at[:, 0:D - D_OWN], recv_sem.at[6])
            x_team[...] = xb_team[...].astype(F32)
        else:
            gather_all(x_block, LAYERS, norm_final[...], lambda half: None)

    head_load.wait()
    copies = []
    for i, first in enumerate(range(0, VOCAB_OWN, HEAD_CHUNK)):
        size = min(HEAD_CHUNK, VOCAB_OWN - first)
        logits[first:first + size, :] = dot_f32(head_buf[first:first + size, :], g_buf[...], ((1,), (1,)))
        copies.append(pltpu.make_async_copy(logits.at[first:first + size], out.at[first:first + size], out_sem.at[i]))
        copies[-1].start()
    for copy in copies:
        copy.wait()
    for ref, sem in pending:
        wait_bytes(ref, sem)


def make_selectors(pack, spread):
    row = lax.broadcasted_iota(jnp.int32, pack.shape, 0)
    col = lax.broadcasted_iota(jnp.int32, pack.shape, 1)
    half = jnp.where(row >= HEADS, 1, 0)
    head = row - HEADS * half
    hit = col == half * 32 + (head & 1) * 16 + (head >> 1)
    pack[...] = jnp.where(hit, 1.0, 0.0).astype(BF16)
    shape = (TEAM_ROWS, TEAM_ROWS * O_ROWS)
    row = lax.broadcasted_iota(jnp.int32, shape, 0)
    col = lax.broadcasted_iota(jnp.int32, shape, 1)
    at = col - row * O_ROWS
    for i in range(O_ROWS):
        wanted = (i % 2) * HEADS + i // 2
        spread[i * TEAM_ROWS:(i + 1) * TEAM_ROWS, :] = jnp.where(at == wanted, 1.0, 0.0).astype(BF16)


def decode(hidden, lengths, kv_cache, norm_attn, w_q, w_o, norm_ffn, w_gate, w_up, w_down, norm_final, w_head):
    hbm = pl.BlockSpec(memory_space=pl.ANY)
    dma = pltpu.SemaphoreType.DMA
    return pl.pallas_call(
        decode_kernel,
        out_shape=jax.ShapeDtypeStruct((VOCAB_OWN, ALL_ROWS), F32),
        in_specs=[hbm] * 12,
        out_specs=hbm,
        scratch_shapes=[
            pltpu.VMEM((ROWS, D), BF16),
            pltpu.SMEM((ROWS,), jnp.int32),
            pltpu.VMEM((LAYERS, D), F32),
            pltpu.VMEM((LAYERS, D), F32),
            pltpu.VMEM((1, D), F32),
            pltpu.VMEM((VOCAB_OWN, D), BF16),
            pltpu.VMEM((VOCAB_OWN, ALL_ROWS), F32),
            pltpu.VMEM((O_ROWS, 64), BF16),
            pltpu.VMEM((O_ROWS * TEAM_ROWS, TEAM_ROWS * O_ROWS), BF16),
            pltpu.VMEM((TEAM, ROWS, D), BF16),
            pltpu.VMEM((TEAM_ROWS, D), F32),
            pltpu.VMEM((TEAM_ROWS, D), BF16),
            pltpu.VMEM((LAYERS, D, Q_OWN), BF16),
            pltpu.VMEM((LAYERS, ROWS, KV + 2 * SHIFT, SEQ), BF16),
            pltpu.VMEM((LAYERS, HEADS * LATENT, D_OWN), BF16),
            pltpu.VMEM((LAYERS, 2 * F_OWN, D), BF16),
            pltpu.VMEM((LAYERS, F_TEAM, D_OWN), BF16),
            pltpu.VMEM((LAYERS, TEAM, ROWS, Q_OWN), BF16),
            pltpu.VMEM((LAYERS, TEAM, ROWS, Q_OWN), BF16),
            pltpu.VMEM((ROWS, 16, PAIR), F32),
            pltpu.VMEM((LAYERS, ROWS, O_ROWS, O_COLS), BF16),
            pltpu.VMEM((LAYERS, TEAM, ROWS, O_ROWS, O_COLS), BF16),
            pltpu.VMEM((O_ROWS * TEAM_ROWS, O_COLS), BF16),
            pltpu.VMEM((LAYERS + 1, TEAMS, TEAM_ROWS, D), BF16),
            pltpu.VMEM((ALL_ROWS, D), BF16),
            pltpu.VMEM((LAYERS, F_TEAM, ALL_ROWS), BF16),
            pltpu.VMEM((LAYERS, TEAMS, TEAM_ROWS, D_OWN), F32),
            pltpu.VMEM((LAYERS, TEAMS, TEAM_ROWS, D_OWN), F32),
            dma((LAYERS, 6)),
            pltpu.SemaphoreType.REGULAR,
            dma((22,)),
            dma((22,)),
            dma((LAYERS + 1, 8)),
            dma((LAYERS,)),
            dma((LAYERS,)),
            dma((LAYERS, ROWS, 3)),
            dma,
            dma((-(-VOCAB_OWN // HEAD_CHUNK),)),
            dma((5,)),
        ],
        compiler_params=pltpu.CompilerParams(collective_id=0, has_side_effects=True, vmem_limit_bytes=60 * 1024 * 1024),
        name='decode',
    )(hidden, lengths, kv_cache, norm_attn, w_q, w_o, norm_ffn, w_gate, w_up, w_down, norm_final, w_head)


def solution(mesh):
    row_axes = ('rep', 'dp')
    specs_in = (P(row_axes, None), P(row_axes), P(None, row_axes, None, None), P(), P(), P(), P(),
                P(None, None, 'dp'), P(None, None, 'dp'), P(None, 'dp', None), P(), P(None, 'dp'))

    def device_step(hidden, lengths, kv_cache, norm_attn, w_q, w_o, norm_ffn, w_gate, w_up, w_down, norm_final, w_head):
        logits = decode(hidden, lengths, jnp.swapaxes(kv_cache, 2, 3), norm_attn, w_q, w_o, norm_ffn,
                        jnp.swapaxes(w_gate, 1, 2), jnp.swapaxes(w_up, 1, 2), w_down, norm_final.reshape(1, -1),
                        jnp.swapaxes(w_head, 0, 1))
        return jnp.swapaxes(logits, 0, 1)

    return jax.shard_map(device_step, mesh=mesh, in_specs=specs_in, out_specs=P('rep', 'dp'), check_vma=False)
```
